32 devices in a mesh: grp: 2 (over y), dp: 16 (over z, x, core).
Axes of the slice: x: 2, y: 2, z: 4, core: 2. Of those that a mesh axis runs over, the one named last changes fastest.
Arguments:
- params: float32 [1900544], P(('grp', 'dp')), parts along dimension 0, may hold values from -0.3 to 0.3
- momentum: float32 [1900544], P(('grp', 'dp')), parts along dimension 0, may hold values from -6 to 6
- noise_draws: float32 [2, 950272], P('grp', 'dp'), parts along dimension 0, may hold values from -6 to 6
- images: float32 [16384, 448], P(('grp', 'dp')), parts along dimension 0, may hold values from -6 to 6
- labels: int32 [16384], P(('grp', 'dp')), parts along dimension 0, may hold values from 0 to 9
- indices: int32 [2, 4096], P('grp', 'dp'), parts along dimension 0, may hold values from 0 to 511
Outputs:
- params_out: float32 [1900544], P(('grp', 'dp')), parts along dimension 0
- momentum_out: float32 [1900544], P(('grp', 'dp')), parts along dimension 0
- losses: float32 [2], P('grp'), parts along dimension 0
The draws below stay inside these ranges and needn't reach their ends.
There are 2 independent parts, one for each index of `grp`. The reference program is written for one: setup_inputs(seed, part) draws one part's arguments, and reference() takes and returns one part's arrays. A program takes and returns all parts, laid end to end along the dimension named above; each array names one. Nothing has to cross between parts.
All inputs are finite; a program needn't handle non-finite values.
Results may differ from the reference program's by a relative error of at most 0.0003.
Values sent between devices are 32-bit elements; how exact they have to be, the bound alone decides.
No kernel may reach another device: no remote copies, remote signals or barrier semaphores. Data moves between devices by JAX's collectives and lax.ppermute only.
A program may use at most 64 MiB of HBM per device.

```python
import math
import jax
import jax.numpy as jnp
from jax import lax

DIN = 448
H = 2048
OUT = 10
POOL_DEV = 512
BATCH_DEV = 256
STEPS = 1
PARAMS = 950272
POOL = 8192
BATCH = 4096
N_DP = 16


def place_ends(drawn, own_key, least, high):
    extent = drawn.shape
    spot = [jax.random.randint(jax.random.fold_in(own_key, axis), (), 0, extent[axis]) for axis in range(len(extent))]
    drawn = drawn.at[tuple(spot)].set(least)
    longest = extent.index(max(extent))
    spot[longest] = (spot[longest] + 1) % extent[longest]
    return drawn.at[tuple(spot)].set(high)


def shard_levels(key, extent, pieces, least, largest):
    def one(axis_at, parts):
        steps = jax.random.uniform(jax.random.fold_in(jax.random.fold_in(key, 6), axis_at), (parts,), jnp.float32, least / len(pieces), largest / len(pieces))
        return jnp.repeat(jnp.exp(steps), extent[axis_at] // parts).reshape((-1,) + (1,) * (len(extent) - axis_at - 1))

    level = one(*pieces[0])
    for cut in pieces[1:]:
        level = level * one(*cut)
    return level


def centred(key, extent, scale, bound, shards=(), kind=jnp.bfloat16):
    values = jax.random.normal(key, extent, jnp.float32) * scale
    if len(shards) > 0:
        values = shard_levels(key, extent, shards, -0.22, 0.18) * values
    return jnp.clip(values, min=-bound, max=bound).astype(kind)


def setup_inputs(seed: int = 0, part: int = 0) -> dict:
    seeds = jax.random.split(jax.random.key(seed), 7)
    own_keys = jax.random.split(jax.random.fold_in(seeds[6], part), 7)
    params = centred(own_keys[0], (PARAMS,), 0.05, 0.3, ((0, 16),), jnp.float32)
    momentum = centred(own_keys[1], (PARAMS,), 1.0, 6.0, ((0, 16),), jnp.float32)
    noise_draws = centred(own_keys[2], (STEPS, PARAMS), 1.0, 6.0, ((1, 16),), jnp.float32)
    images = centred(own_keys[3], (POOL, DIN), 1.0, 6.0, ((0, 16),), jnp.float32)
    labels = place_ends(jax.random.randint(own_keys[4], (POOL,), 0, OUT), jax.random.fold_in(own_keys[4], 1), 0, OUT - 1).astype(jnp.int32)
    indices = place_ends(jax.random.randint(own_keys[5], (STEPS, BATCH), 0, POOL_DEV), jax.random.fold_in(own_keys[5], 1), 0, POOL_DEV - 1).astype(jnp.int32)
    return {"params": params, "momentum": momentum, "noise_draws": noise_draws, "images": images, "labels": labels, "indices": indices}


step_size = 0.02
friction = 15.0

def unpack(flat_vec):
    in_end = DIN * H
    w_in = flat_vec[:in_end].reshape(DIN, H)
    b_in = flat_vec[in_end:in_end + H]
    hid_end = in_end + H
    w_out = flat_vec[hid_end:hid_end + H * OUT].reshape(H, OUT)
    b_out = flat_vec[hid_end + H * OUT:hid_end + H * OUT + OUT]
    return (w_in, b_in, w_out, b_out)

def total_nll(flat_vec, chosen_rows, targets):
    w_in, b_in, w_out, b_out = unpack(flat_vec)
    hidden = jnp.tanh(jnp.dot(chosen_rows, w_in, precision=lax.Precision.HIGHEST, preferred_element_type=jnp.float32) + b_in)
    logits = jnp.dot(hidden, w_out, precision=lax.Precision.HIGHEST, preferred_element_type=jnp.float32) + b_out
    log_norm = jnp.log(lax.optimization_barrier(jnp.sum(jnp.exp(logits), axis=1)))
    classes = lax.broadcasted_iota(jnp.int32, logits.shape, 1)
    picked = lax.optimization_barrier(jnp.sum(jnp.where(targets[:, None] == classes, logits, 0.0), axis=1))
    return jnp.sum(log_norm - picked)

def prior_precision(flat_index):
    in_end = DIN * H
    hid_end = in_end + H
    out_end = hid_end + H * OUT
    return jnp.where(flat_index < in_end, float(DIN), jnp.where(flat_index < hid_end, 1.0, jnp.where(flat_index < out_end, float(H), 1.0)))

def reference(params, momentum, noise_draws, images, labels, indices):
    offsets = jnp.arange(BATCH, dtype=jnp.int32) // BATCH_DEV * POOL_DEV
    precision = prior_precision(jnp.arange(PARAMS, dtype=jnp.int32))
    losses = []
    for step_idx in range(STEPS):
        pool_rows = (indices[step_idx].astype(jnp.int32) + offsets).astype(jnp.int32)
        blocks = pool_rows.reshape(N_DP, BATCH_DEV)

        def one_block(carry, block):
            chosen_rows = images[block]
            targets = labels[block]
            nll_part, pullback = jax.vjp(lambda weights_flat: total_nll(weights_flat, chosen_rows, targets), params)
            local_grad, = pullback(jnp.ones_like(nll_part))
            return ((carry[0] + local_grad, carry[1] + nll_part), None)
        start_carry = (jnp.zeros((PARAMS,), jnp.float32), jnp.zeros((), jnp.float32))
        (grad_sum, nll_sum), _ = lax.scan(one_block, start_carry, blocks)
        losses.append(nll_sum / BATCH)
        total_force = POOL / BATCH * grad_sum + precision * params
        momentum = (1.0 - step_size * friction) * momentum - step_size * total_force + math.sqrt(2.0 * friction * step_size) * noise_draws[step_idx]
        params = params + step_size * momentum
    return (params, momentum, jnp.stack(losses))
```

```python
import functools
import math

import jax
import jax.numpy as jnp
from jax import lax
from jax.experimental import pallas as pl
from jax.experimental.pallas import tpu as pltpu
from jax.sharding import PartitionSpec as P

H = 2048
OUT = 10
LANES = 128
COPIES = 2

step_size = 0.02
friction = 15.0
F32, BF16 = jnp.float32, jnp.bfloat16


def up8(n):
    return -(-n // 8) * 8


class Plan:
    def __init__(self, devices, din, shard_len, batch):
        self.n = devices
        self.group = devices // COPIES
        self.din = din
        self.cols = H // self.group
        self.nb = self.cols // LANES
        self.rows = shard_len // H
        self.pad = up8(self.rows + 1)
        self.step = H // LANES
        self.flat = shard_len // LANES
        self.batch = batch
        self.tail = din + 1 - (devices - 1) * self.rows
        self.k = devices * self.pad
        gcd = math.gcd(LANES, OUT)
        self.hp, self.qp = LANES // gcd, OUT // gcd
        self.periods = self.cols // self.hp
        self.classes = up8(OUT)
        self.xrows = up8(din + 1)

    @staticmethod
    def fits(devices, din, shard_len, batch):
        if devices & (devices - 1) or devices < 2 * COPIES or shard_len % (8 * LANES) or shard_len % H:
            return False
        group, rows = devices // COPIES, shard_len // H
        if H % (group * LANES) or batch % LANES or din % 8:
            return False
        tail = din + 1 - (devices - 1) * rows
        return 0 < tail and tail + OUT + 1 <= rows


def split(x):
    hi = x.astype(BF16)
    return hi, (x - hi.astype(F32)).astype(BF16)


def split3(x):
    hi = x.astype(BF16)
    rest = x - hi.astype(F32)
    mid = rest.astype(BF16)
    return hi, mid, (rest - mid.astype(F32)).astype(BF16)


def dot(a, b, dims):
    return lax.dot_general(a, b, (dims, ((), ())), preferred_element_type=F32)


NN, NT, TN = ((1,), (0,)), ((1,), (1,)), ((0,), (0,))


def dot3(a, b, dims):
    return dot(a[0], b[0], dims) + (dot(a[0], b[1], dims) + dot(a[1], b[0], dims))


def iota(shape, axis):
    return lax.broadcasted_iota(jnp.int32, shape, axis)


def gather_kernel(plan, img_ref, lab_ref, idx_ref, out_ref):
    pool = img_ref.shape[1]
    hot = (iota((pool, plan.batch), 0) == idx_ref[...]).astype(BF16)
    hi, mid, lo = split3(img_ref[...])
    out_ref[: plan.din, :] = dot(hi, hot, NN) + dot(mid, hot, NN) + dot(lo, hot, NN)
    lab = jnp.broadcast_to(lab_ref[...].astype(F32), (plan.xrows - plan.din, pool)).astype(BF16)
    out_ref[plan.din :, :] = dot(lab, hot, NN)


def cut_kernel(plan, last_ref, par_ref, out_ref):
    out_ref[...] = jnp.zeros_like(out_ref)
    for j in range(plan.group):
        for b in range(plan.nb):
            piece = par_ref[pl.ds(j * plan.nb + b, plan.rows, stride=plan.step), :]
            for d in range(j, plan.n, plan.group):
                out_ref[d, : plan.rows, b * LANES : (b + 1) * LANES] = piece

    @pl.when(last_ref[0] == 1)
    def _():
        t = plan.tail
        for j in range(plan.group):
            for d in range(j, plan.n, plan.group):
                out_ref[d, t + OUT, :LANES] = par_ref[(t + OUT) * plan.step, :]
            for b in range(plan.nb):
                start = t * plan.step + j * plan.nb * OUT + b
                piece = par_ref[pl.ds(start, OUT, stride=plan.nb), :]
                for d in range(j, plan.n, plan.group):
                    out_ref[d, t : t + OUT, b * LANES : (b + 1) * LANES] = piece


def class_masks(plan):
    width = plan.qp * LANES
    mask = (iota((plan.classes, width), 1) % OUT == iota((plan.classes, width), 0)).astype(F32)
    place = (iota((width, plan.hp), 0) // OUT == iota((width, plan.hp), 1)).astype(BF16)
    return mask, place


def flat_spot(plan, r):
    row = (plan.n - 1) * plan.pad + plan.tail + r // plan.nb
    col = r % plan.nb * LANES
    return row, col


def forward_kernel(plan, w_ref, *refs):
    x_refs, (xh_ref, xl_ref, h_ref, a_ref, lg_ref), pad_ref = refs[: plan.group], refs[plan.group : -1], refs[-1]
    mask, place = class_masks(plan)
    for p in range(plan.periods):
        parts = []
        for q in range(plan.qp):
            row, col = flat_spot(plan, p * plan.qp + q)
            parts.append(jnp.broadcast_to(w_ref[row : row + 1, col : col + LANES], (plan.classes, LANES)))
        lhs = jnp.concatenate(parts, axis=1) * mask
        hi, mid, lo = split3(lhs)
        a_ref[:, p * plan.hp : (p + 1) * plan.hp] = dot(hi, place, NN) + dot(mid, place, NN) + dot(lo, place, NN)
    a = split(a_ref[...])
    wt = split(w_ref[...].T)
    pad_ref[...] = jnp.zeros_like(pad_ref)
    one = (plan.n - 1) * plan.pad + plan.tail - 1
    pad_ref[one : one + 1, :] = jnp.ones((1, plan.batch), F32)
    for m in range(plan.group):
        here = slice(m * plan.batch, (m + 1) * plan.batch)
        for d in range(plan.n):
            count = min(plan.rows, plan.din - d * plan.rows)
            pad_ref[d * plan.pad : d * plan.pad + count, :] = x_refs[m][d * plan.rows : d * plan.rows + count, :]
        xs = split(pad_ref[...])
        xh_ref[:, here] = xs[0]
        xl_ref[:, here] = xs[1]
        hidden = jnp.tanh(dot3(wt, xs, NN))
        h_ref[:, here] = hidden
        lg_ref[:, here] = dot3(a, split(hidden), NN)


def backward_kernel(plan, lg_ref, lab_ref, w_ref, a_ref, xh_ref, xl_ref, h_ref, out_ref, dh_ref, dl_ref):
    total = plan.group * plan.batch
    diag = iota((plan.classes, LANES), 0) == iota((plan.classes, LANES), 1)
    row = (plan.n - 1) * plan.pad + plan.tail + OUT
    bias = jnp.sum(jnp.where(diag, w_ref[row : row + 1, :LANES], 0.0), axis=1, keepdims=True)
    logits = lg_ref[...] + bias
    kind = iota((plan.classes, total), 0)
    logits = jnp.where(kind < OUT, logits, -jnp.inf)
    top = jnp.max(logits, axis=0, keepdims=True)
    ex = jnp.exp(logits - top)
    norm = jnp.sum(ex, axis=0, keepdims=True)
    hit = kind == lab_ref[...].astype(jnp.int32)
    picked = jnp.sum(jnp.where(hit, logits, 0.0), axis=0, keepdims=True)
    nll = jnp.sum(jnp.log(norm) + top - picked, axis=1, keepdims=True)
    dl = ex / norm - jnp.where(hit, 1.0, 0.0)
    dbias = jnp.sum(dl, axis=1, keepdims=True)
    dbias = jnp.sum(jnp.where(diag, dbias, 0.0), axis=0, keepdims=True)
    dl_ref[...] = dl
    a = split(a_ref[...])
    da = jnp.zeros((plan.classes, plan.cols), F32)
    dw = jnp.zeros((plan.k, plan.cols), F32)
    for m in range(plan.group):
        here = slice(m * plan.batch, (m + 1) * plan.batch)
        dls = split(dl_ref[:, here])
        hidden = h_ref[:, here]
        dh = split(dot3(a, dls, TN) * (1.0 - hidden * hidden))
        dh_ref[0, :, here] = dh[0]
        dh_ref[1, :, here] = dh[1]
        da = da + dot3(dls, split(hidden), NT)
    dhs = (dh_ref[0], dh_ref[1])
    for d in range(0, plan.n, 2):
        here = slice(d * plan.pad, (d + 2) * plan.pad)
        dw = dot3((xh_ref[here, :], xl_ref[here, :]), dhs, NT)
        out_ref[here, :] = dw
    mask, place = class_masks(plan)
    for p in range(plan.periods):
        hi, mid, lo = split3(da[:, p * plan.hp : (p + 1) * plan.hp])
        back = dot(hi, place, NT) + dot(mid, place, NT) + dot(lo, place, NT)
        back = jnp.sum(back * mask, axis=0, keepdims=True)
        for q in range(plan.qp):
            r, c = flat_spot(plan, p * plan.qp + q)
            out_ref[r : r + 1, c : c + LANES] = back[:, q * LANES : (q + 1) * LANES]
    out_ref[row : row + 1, :LANES] = dbias
    for d in range(plan.n):
        at = d * plan.pad + plan.rows
        out_ref[at : at + 1, :LANES] = jnp.broadcast_to(nll, (1, LANES))


def update_kernel(plan, scale, count, at_ref, got_ref, par_ref, mom_ref, noise_ref, par_out, mom_out, loss_ref, grad_ref):
    loss = jnp.zeros((1, LANES), F32)
    t = plan.tail
    pieces = []
    for j in range(plan.group):
        piece = got_ref[j * plan.pad : (j + 1) * plan.pad, :]
        for g in range(1, COPIES):
            at = (g * plan.group + j) * plan.pad
            piece = piece + got_ref[at : at + plan.pad, :]
        pieces.append(piece)
        for b in range(plan.nb):
            lanes = slice(b * LANES, (b + 1) * LANES)
            grad_ref[pl.ds(j * plan.nb + b, plan.rows, stride=plan.step), :] = piece[: plan.rows, lanes]
    loss_ref[...] = pieces[0][plan.rows : plan.rows + 1, :LANES] * (1.0 / count)

    @pl.when(at_ref[1] == 1)
    def _():
        grad_ref[(t + OUT) * plan.step :, :] = jnp.zeros((plan.flat - (t + OUT) * plan.step, LANES), F32)
        row = (t + OUT) * plan.step
        grad_ref[row : row + 1, :] = pieces[0][t + OUT : t + OUT + 1, :LANES]
        for j in range(plan.group):
            for b in range(plan.nb):
                lanes = slice(b * LANES, (b + 1) * LANES)
                start = t * plan.step + j * plan.nb * OUT + b
                grad_ref[pl.ds(start, OUT, stride=plan.nb), :] = pieces[j][t : t + OUT, lanes]

    shape = (plan.flat, LANES)
    index = at_ref[0] + iota(shape, 0) * LANES + iota(shape, 1)
    prec = precision_of(index, plan.din)
    old = par_ref[...]
    force = scale * grad_ref[...] + prec * old
    mom = (1.0 - step_size * friction) * mom_ref[...] - step_size * force
    mom = mom + math.sqrt(2.0 * friction * step_size) * noise_ref[...]
    mom_out[...] = mom
    par_out[...] = old + step_size * mom


def precision_of(index, din):
    in_end = din * H
    hid_end = in_end + H
    out_end = hid_end + H * OUT
    inner = jnp.where(index < hid_end, 1.0, jnp.where(index < out_end, float(H), 1.0))
    return jnp.where(index < in_end, float(din), inner)


def call(kernel, args, outs, scratch=(), smem=0):
    vm = pl.BlockSpec(memory_space=pltpu.VMEM)
    sm = pl.BlockSpec(memory_space=pltpu.SMEM)
    size = sum(math.prod(s) for s, _ in outs)
    return pl.pallas_call(
        kernel,
        out_shape=[jax.ShapeDtypeStruct(s, t) for s, t in outs],
        in_specs=[sm] * smem + [vm] * (len(args) - smem),
        out_specs=[vm] * len(outs),
        scratch_shapes=list(scratch),
        cost_estimate=pl.CostEstimate(flops=1000 * size, bytes_accessed=8 * size, transcendentals=0),
    )(*args)


def fast_body(n, params, momentum, noise_draws, images, labels, indices):
    pool, din = images.shape
    plan = Plan(n, din, params.shape[0], indices.shape[1])
    me = lax.axis_index("dp")
    last = (me == n - 1).astype(jnp.int32)
    flat = (plan.flat, LANES)
    tall = (n * plan.pad, plan.cols)
    hop = lambda x, k: lax.ppermute(x, "dp", [(d, d ^ k) for d in range(n)])

    (rows,) = call(
        functools.partial(gather_kernel, plan),
        (images.T, labels.reshape(1, pool), indices),
        [((plan.xrows, plan.batch), F32)],
    )
    xs = [rows] + [hop(rows, m) for m in range(2, plan.group, 2)]
    (cut,) = call(
        functools.partial(cut_kernel, plan),
        (last.reshape(1), params.reshape(flat)),
        [((n, plan.pad, plan.cols), F32)],
        smem=1,
    )
    weights = lax.all_to_all(cut.reshape(tall), "dp", 0, 0, tiled=True)
    others = [hop(x, 1) for x in xs]
    slots = [y for pair in zip(xs, others) for y in pair]
    total = plan.group * plan.batch
    xh, xl, hidden, outw, logits = call(
        functools.partial(forward_kernel, plan),
        (weights, *slots),
        [
            ((plan.k, total), BF16),
            ((plan.k, total), BF16),
            ((plan.cols, total), F32),
            ((plan.classes, plan.cols), F32),
            ((plan.classes, total), F32),
        ],
        [pltpu.VMEM((plan.k, plan.batch), F32)],
    )

    def moved(x, k):
        got = hop(x, k)
        return jnp.concatenate([got[:, (m ^ k) * plan.batch : ((m ^ k) + 1) * plan.batch] for m in range(plan.group)], 1)

    k = 1
    while k < plan.group:
        logits = logits + moved(logits, k)
        k *= 2
    marks = jnp.concatenate([s[din : din + 1] for s in slots], axis=1)
    (grads,) = call(
        functools.partial(backward_kernel, plan),
        (logits, marks, weights, outw, xh, xl, hidden),
        [(tall, F32)],
        [pltpu.VMEM((2, plan.cols, total), BF16), pltpu.VMEM((plan.classes, total), F32)],
    )
    got = lax.all_to_all(grads, "dp", 0, 0, tiled=True)
    scale = pool / plan.batch
    count = n * plan.batch
    new_params, new_momentum, loss = call(
        functools.partial(update_kernel, plan, scale, count),
        (
            jnp.stack([me * params.shape[0], last]),
            got,
            params.reshape(flat),
            momentum.reshape(flat),
            noise_draws.reshape(flat),
        ),
        [(flat, F32), (flat, F32), ((1, LANES), F32)],
        [pltpu.VMEM(flat, F32)],
        smem=1,
    )
    return new_params.reshape(-1), new_momentum.reshape(-1), loss[0, :1]


def total_nll(flat_vec, din, chosen_rows, targets):
    in_end = din * H
    hid_end = in_end + H
    w_in = flat_vec[:in_end].reshape(din, H)
    b_in = flat_vec[in_end:hid_end]
    w_out = flat_vec[hid_end : hid_end + H * OUT].reshape(H, OUT)
    b_out = flat_vec[hid_end + H * OUT : hid_end + H * OUT + OUT]
    high = dict(precision=lax.Precision.HIGHEST, preferred_element_type=F32)
    hidden = jnp.tanh(jnp.dot(chosen_rows, w_in, **high) + b_in)
    logits = jnp.dot(hidden, w_out, **high) + b_out
    log_norm = jnp.log(jnp.sum(jnp.exp(logits), axis=1))
    classes = iota(logits.shape, 1)
    picked = jnp.sum(jnp.where(targets[:, None] == classes, logits, 0.0), axis=1)
    return jnp.sum(log_norm - picked)


def plain_body(params, momentum, noise_draws, images, labels, indices):
    shard_len = params.shape[0]
    din = images.shape[1]
    shard_start = lax.axis_index("dp") * shard_len
    precision = precision_of(shard_start + lax.iota(jnp.int32, shard_len), din)
    gathered = lax.all_gather(params, "dp", axis=0, tiled=True)
    chosen_rows = jnp.take(images, indices[0], axis=0)
    targets = jnp.take(labels, indices[0], axis=0)
    nll, pullback = jax.vjp(lambda w: total_nll(w, din, chosen_rows, targets), gathered)
    (local_grad,) = pullback(jnp.ones_like(nll))
    loss = lax.psum(nll, "dp") / (lax.axis_size("dp") * indices.shape[1])
    own_grad = lax.psum_scatter(local_grad, "dp", scatter_dimension=0, tiled=True)
    force = images.shape[0] / indices.shape[1] * own_grad + precision * params
    momentum = (1.0 - step_size * friction) * momentum - step_size * force
    momentum = momentum + math.sqrt(2.0 * friction * step_size) * noise_draws[0]
    return params + step_size * momentum, momentum, loss.reshape(1)


def solution(mesh):
    n = mesh.shape["dp"]

    def body(*args):
        params, images, indices = args[0], args[3], args[5]
        if Plan.fits(n, images.shape[1], params.shape[0], indices.shape[1]):
            return fast_body(n, *args)
        return plain_body(*args)

    placed = (
        P(("grp", "dp")),
        P(("grp", "dp")),
        P("grp", "dp"),
        P(("grp", "dp"), None),
        P(("grp", "dp")),
        P("grp", "dp"),
    )
    return jax.shard_map(
        body,
        mesh=mesh,
        in_specs=placed,
        out_specs=(P(("grp", "dp")), P(("grp", "dp")), P("grp")),
        check_vma=False,
    )
```

```python
import functools
import math

import jax
import jax.numpy as jnp
from jax import lax
from jax.experimental import pallas as pl
from jax.experimental.pallas import tpu as pltpu
from jax.sharding import PartitionSpec as P


H = 2048
OUT = 10
LANES = 128
LIMIT = 16
COPIES = 2

step_size = 0.02
friction = 15.0
F32, BF16 = jnp.float32, jnp.bfloat16


def up8(n):
    return -(-n // 8) * 8


class Plan:
    def __init__(self, devices, din, shard_len, batch):
        self.n = devices
        self.group = devices // COPIES
        self.din = din
        self.cols = H // self.group
        self.nb = self.cols // LANES
        self.rows = shard_len // H
        self.pad = up8(self.rows + 1)
        self.step = H // LANES
        self.flat = shard_len // LANES
        self.batch = batch
        self.half = batch // 2
        self.tail = din + 1 - (devices - 1) * self.rows
        gcd = math.gcd(LANES, OUT)
        self.hp, self.qp = LANES // gcd, OUT // gcd
        self.periods = self.cols // self.hp
        self.classes = up8(OUT)
        self.xrows = -(-(din + 2) // 16) * 16

    @staticmethod
    def fits(devices, din, shard_len, batch):
        if devices & (devices - 1) or devices < 2 * COPIES or shard_len % (8 * LANES) or shard_len % H:
            return False
        group, rows = devices // COPIES, shard_len // H
        if H % (group * LANES) or batch % (2 * LANES) or group not in (4, 8) or din % 8:
            return False
        tail = din + 1 - (devices - 1) * rows
        return 0 < tail and tail + OUT + 1 <= rows


def split(x):
    hi = x.astype(BF16)
    return hi, (x - hi.astype(F32)).astype(BF16)


def split3(x):
    hi = x.astype(BF16)
    rest = x - hi.astype(F32)
    mid = rest.astype(BF16)
    return hi, mid, (rest - mid.astype(F32)).astype(BF16)


def dot(a, b, dims):
    return lax.dot_general(a, b, (dims, ((), ())), preferred_element_type=F32)


NN, NT = ((1,), (0,)), ((1,), (1,))


def iota(shape, axis):
    return lax.broadcasted_iota(jnp.int32, shape, axis)


def pick_kernel(plan, img_ref, lab_ref, idx_ref, *refs):
    parts, (img, lab, idx, sems) = refs[:-4], refs[-4:]
    loads = [pltpu.make_async_copy(s, d, sems.at[i]) for i, (s, d) in enumerate(
        ((idx_ref, idx), (lab_ref, lab), (img_ref, img)))]
    for load in loads:
        load.start()
    for load in loads:
        load.wait()
    pool = img.shape[1]
    hot = (iota((pool, plan.batch), 0) == idx[...]).astype(BF16)
    hi, mid, lo = split3(img[...])
    rows = dot(hi, hot, NN) + dot(mid, hot, NN) + dot(lo, hot, NN)
    spare = plan.xrows - plan.din
    marks = jnp.broadcast_to(lab[...].astype(F32), (spare, pool)).astype(BF16)
    marks = dot(marks, hot, NN)
    at = iota((spare, plan.batch), 0)
    marks = jnp.where(at == 0, 1.0, jnp.where(at == 1, marks, 0.0))
    for i, part in enumerate(parts):
        part[: plan.din, :] = rows[:, i * plan.half : (i + 1) * plan.half]
        part[plan.din :, :] = marks[:, i * plan.half : (i + 1) * plan.half]


def cut_kernel(plan, last_ref, par_ref, out_ref):
    cut_weights(plan, last_ref, par_ref, out_ref)


def cut_weights(plan, last_ref, par_ref, out_ref):
    out_ref[...] = jnp.zeros_like(out_ref)
    for j in range(plan.group):
        for b in range(plan.nb):
            piece = par_ref[pl.ds(j * plan.nb + b, plan.rows, stride=plan.step), :]
            for d in range(j, plan.n, plan.group):
                out_ref[d, : plan.rows, b * LANES : (b + 1) * LANES] = piece

    @pl.when(last_ref[0] == 1)
    def _():
        t = plan.tail
        for j in range(plan.group):
            for d in range(j, plan.n, plan.group):
                out_ref[d, t + OUT, :LANES] = par_ref[(t + OUT) * plan.step, :]
            for b in range(plan.nb):
                start = t * plan.step + j * plan.nb * OUT + b
                piece = par_ref[pl.ds(start, OUT, stride=plan.nb), :]
                for d in range(j, plan.n, plan.group):
                    out_ref[d, t : t + OUT, b * LANES : (b + 1) * LANES] = piece


def class_masks(plan):
    width = plan.qp * LANES
    mask = (iota((plan.classes, width), 1) % OUT == iota((plan.classes, width), 0)).astype(F32)
    place = (iota((width, plan.hp), 0) // OUT == iota((width, plan.hp), 1)).astype(BF16)
    return mask, place


def flat_spot(plan, r):
    row = (plan.n - 1) * plan.pad + plan.tail + r // plan.nb
    col = r % plan.nb * LANES
    return row, col


def blocks_of(plan):
    return [(d, d * plan.rows, min(plan.rows, plan.din + 1 - d * plan.rows)) for d in range(plan.n)]


def forward_kernel(plan, w_ref, *refs):
    x_refs = refs[: 2 * plan.group]
    x_ref, h_ref, a_ref, own_ref, send_ref, lab_ref, c_ref = refs[2 * plan.group :]
    mask, place = class_masks(plan)
    lhs = []
    for p in range(plan.periods):
        parts = []
        for q in range(plan.qp):
            row, col = flat_spot(plan, p * plan.qp + q)
            parts.append(jnp.broadcast_to(w_ref[row : row + 1, col : col + LANES], (plan.classes, LANES)))
        lhs.append(jnp.concatenate(parts, axis=1) * mask)
    hi, mid, lo = split3(jnp.concatenate(lhs, axis=0))
    out_w = dot(hi, place, NN) + dot(mid, place, NN) + dot(lo, place, NN)
    for p in range(plan.periods):
        rows = slice(p * plan.classes, (p + 1) * plan.classes)
        a_ref[:, p * plan.hp : (p + 1) * plan.hp] = out_w[rows]
    a_hi, a_lo = split(a_ref[...])
    a_cat = jnp.concatenate([a_hi, a_lo], axis=0)
    c_ref[...] = jnp.zeros_like(c_ref)
    for d, first, count in blocks_of(plan):
        c_ref[first : first + count, :] = w_ref[d * plan.pad : d * plan.pad + count, :]
    w_hi, w_lo = split(c_ref[...].T)
    w_cat = jnp.concatenate([w_hi, w_lo], axis=0)
    per = plan.batch // LANES
    for m in range(plan.group):
        here = slice(m * plan.batch, (m + 1) * plan.batch)
        got = jnp.concatenate([x_refs[2 * m][...], x_refs[2 * m + 1][...]], axis=1)
        for i in range(per):
            line = got[plan.din + 1 : plan.din + 2, i * LANES : (i + 1) * LANES]
            lab_ref[m * per + i : m * per + i + 1, :] = line
        x_hi, x_lo = split(got)
        x_ref[: plan.xrows, here] = x_hi
        x_ref[plan.xrows :, here] = x_lo
        pre = dot(w_cat, x_hi, NN)
        hidden = jnp.tanh(pre[: plan.cols] + (pre[plan.cols :] + dot(w_hi, x_lo, NN)))
        h_hi, h_lo = split(hidden)
        h_ref[: plan.cols, here] = h_hi
        h_ref[plan.cols :, here] = h_lo
        lg = dot(a_cat, h_hi, NN)
        lg = lg[: plan.classes] + (lg[plan.classes :] + dot(a_hi, h_lo, NN))
        for i in range(per):
            for o in range(OUT):
                row = lg[o : o + 1, i * LANES : (i + 1) * LANES]
                own_ref[o, m * per + i : m * per + i + 1, :] = row
                send_ref[o, (m ^ 1) * per + i : (m ^ 1) * per + i + 1, :] = row


def backward_kernel(plan, own_ref, w_ref, a_ref, x_ref, h_ref, lab_ref, *refs):
    lg_refs, (out_ref, lg_ref, dl_ref, dh_ref, dw_ref) = refs[:-5], refs[-5:]
    per = plan.batch // LANES
    lines = plan.group * per
    diag = iota((plan.classes, LANES), 0) == iota((plan.classes, LANES), 1)
    row = (plan.n - 1) * plan.pad + plan.tail + OUT
    bias = w_ref[row : row + 1, :LANES]
    for m in range(plan.group):
        value = own_ref[:, m * per : (m + 1) * per, :]
        for i, ref in enumerate(lg_refs):
            other = m ^ (2 * (i + 1))
            value = value + ref[:, other * per : (other + 1) * per, :]
        lg_ref[:, m * per : (m + 1) * per, :] = value
    labels = lab_ref[...].astype(jnp.int32)
    logits = [lg_ref[o] + bias[:, o : o + 1] for o in range(OUT)]
    top = functools.reduce(jnp.maximum, logits)
    ex = [jnp.exp(v - top) for v in logits]
    norm = functools.reduce(jnp.add, ex)
    hits = [labels == o for o in range(OUT)]
    picked = functools.reduce(jnp.add, [jnp.where(h, v, 0.0) for h, v in zip(hits, logits)])
    nll = jnp.sum(jnp.sum(jnp.log(norm) + top - picked, axis=1, keepdims=True), axis=0, keepdims=True)
    share = 1.0 / norm
    dl_ref[...] = jnp.zeros_like(dl_ref)
    for o in range(OUT):
        value = ex[o] * share - jnp.where(hits[o], 1.0, 0.0)
        for i in range(lines):
            dl_ref[o : o + 1, i * LANES : (i + 1) * LANES] = value[i : i + 1, :]
    dl = dl_ref[...]
    dbias = jnp.sum(dl, axis=1, keepdims=True)
    dbias = jnp.sum(jnp.where(diag, dbias, 0.0), axis=0, keepdims=True)
    dl_hi, dl_lo = split(dl)
    at_hi, at_lo = split(a_ref[...].T)
    at_cat = jnp.concatenate([at_hi, at_lo], axis=0)
    for m in range(plan.group):
        here = slice(m * plan.batch, (m + 1) * plan.batch)
        hidden = h_ref[: plan.cols, here].astype(F32) + h_ref[plan.cols :, here].astype(F32)
        dh = dot(at_cat, dl_hi[:, here], NN)
        dh = dh[: plan.cols] + (dh[plan.cols :] + dot(at_hi, dl_lo[:, here], NN))
        dh_hi, dh_lo = split(dh * (1.0 - hidden * hidden))
        dh_ref[: plan.cols, here] = dh_hi
        dh_ref[plan.cols :, here] = dh_lo
    da = dot(h_ref[...], dl_hi, NT)
    da = da[: plan.cols] + (da[plan.cols :] + dot(h_ref[: plan.cols, :], dl_lo, NT))
    dw = dot(x_ref[...], dh_ref[: plan.cols, :], NT)
    dw_ref[...] = dw[: plan.xrows] + (dw[plan.xrows :] + dot(x_ref[: plan.xrows, :], dh_ref[plan.cols :, :], NT))
    out_ref[...] = jnp.zeros_like(out_ref)
    for d, first, count in blocks_of(plan):
        out_ref[d * plan.pad : d * plan.pad + count, :] = dw_ref[first : first + count, :]
    mask, place = class_masks(plan)
    hi, mid, lo = split3(da.T)
    parts = []
    for v in (hi, mid, lo):
        parts.append(jnp.concatenate([v[:, p * plan.hp : (p + 1) * plan.hp] for p in range(plan.periods)], axis=0))
    back = dot(parts[0], place, NT) + dot(parts[1], place, NT) + dot(parts[2], place, NT)
    for p in range(plan.periods):
        line = jnp.sum(back[p * plan.classes : (p + 1) * plan.classes] * mask, axis=0, keepdims=True)
        for q in range(plan.qp):
            r, c = flat_spot(plan, p * plan.qp + q)
            out_ref[r : r + 1, c : c + LANES] = line[:, q * LANES : (q + 1) * LANES]
    out_ref[row : row + 1, :LANES] = dbias
    for d in range(plan.n):
        at = d * plan.pad + plan.rows
        out_ref[at : at + 1, :LANES] = jnp.broadcast_to(nll, (1, LANES))


def prepare_kernel(plan, at_ref, par_ref, mom_ref, noise_ref, base_ref, keep_ref, mom, noise, sems):
    loads = [pltpu.make_async_copy(s, d, sems.at[i]) for i, (s, d) in enumerate(
        ((par_ref, keep_ref), (mom_ref, mom), (noise_ref, noise)))]
    for load in loads:
        load.start()
    for load in loads:
        load.wait()
    shape = (plan.flat, LANES)
    index = at_ref[0] + iota(shape, 0) * LANES + iota(shape, 1)
    prior = precision_of(index, plan.din) * keep_ref[...]
    base = (1.0 - step_size * friction) * mom[...] - step_size * prior
    base_ref[...] = base + math.sqrt(2.0 * friction * step_size) * noise[...]


def update_kernel(plan, scale, count, at_ref, got_ref, base_ref, par_ref, par_out, mom_out, loss_ref, grad_ref):
    t = plan.tail
    pieces = []
    for j in range(plan.group):
        piece = got_ref[j * plan.pad : (j + 1) * plan.pad, :]
        for g in range(1, COPIES):
            at = (g * plan.group + j) * plan.pad
            piece = piece + got_ref[at : at + plan.pad, :]
        pieces.append(piece)
        for b in range(plan.nb):
            lanes = slice(b * LANES, (b + 1) * LANES)
            grad_ref[pl.ds(j * plan.nb + b, plan.rows, stride=plan.step), :] = piece[: plan.rows, lanes]
    loss_ref[...] = pieces[0][plan.rows : plan.rows + 1, :LANES] * (1.0 / count)

    @pl.when(at_ref[1] == 1)
    def _():
        row = (t + OUT) * plan.step
        grad_ref[row:, :] = jnp.zeros((plan.flat - row, LANES), F32)
        grad_ref[row : row + 1, :] = pieces[0][t + OUT : t + OUT + 1, :LANES]
        for j in range(plan.group):
            for b in range(plan.nb):
                lanes = slice(b * LANES, (b + 1) * LANES)
                start = t * plan.step + j * plan.nb * OUT + b
                grad_ref[pl.ds(start, OUT, stride=plan.nb), :] = pieces[j][t : t + OUT, lanes]

    mom = base_ref[...] - (step_size * scale) * grad_ref[...]
    mom_out[...] = mom
    par_out[...] = par_ref[...] + step_size * mom


def precision_of(index, din):
    in_end = din * H
    hid_end = in_end + H
    out_end = hid_end + H * OUT
    inner = jnp.where(index < hid_end, 1.0, jnp.where(index < out_end, float(H), 1.0))
    return jnp.where(index < in_end, float(din), inner)


def call(kernel, args, outs, scratch=(), smem=0, limit=16, whole=0, cost=1):
    vm = pl.BlockSpec(memory_space=pltpu.VMEM)
    sm = pl.BlockSpec(memory_space=pltpu.SMEM)
    anywhere = pl.BlockSpec(memory_space=pltpu.HBM)
    specs = [sm] * smem + [anywhere] * whole
    return pl.pallas_call(
        kernel,
        out_shape=[jax.ShapeDtypeStruct(s, t) for s, t in outs],
        in_specs=specs + [vm] * (len(args) - len(specs)),
        out_specs=[vm] * len(outs),
        scratch_shapes=list(scratch),
        compiler_params=pltpu.CompilerParams(vmem_limit_bytes=limit << 20),
        cost_estimate=pl.CostEstimate(flops=cost * 10**9, bytes_accessed=1 << 20, transcendentals=0),
    )(*args)


def fast_body(n, params, momentum, noise_draws, images, labels, indices):
    pool, din = images.shape
    plan = Plan(n, din, params.shape[0], indices.shape[1])
    me = lax.axis_index("dp")
    last = (me == n - 1).astype(jnp.int32)
    flat = (plan.flat, LANES)
    tall = (n * plan.pad, plan.cols)
    total = plan.group * plan.batch
    dense = (OUT, total // LANES, LANES)

    def hop(x, k):
        return lax.ppermute(x, "dp", [(d, d ^ k) for d in range(n)])


    rows = call(
        functools.partial(pick_kernel, plan),
        (images.T, labels.reshape(1, pool), indices),
        [((plan.xrows, plan.half), F32)] * 2,
        [
            pltpu.VMEM((din, pool), F32),
            pltpu.VMEM((1, pool), jnp.int32),
            pltpu.VMEM((1, plan.batch), jnp.int32),
            pltpu.SemaphoreType.DMA((3,)),
        ],
        whole=3,
        limit=LIMIT,
    )
    *rows, mine = lax.optimization_barrier((*rows, params))
    (cut,) = call(
        functools.partial(cut_kernel, plan),
        (last.reshape(1), mine.reshape(flat)),
        [((n, plan.pad, plan.cols), F32)],
        smem=1,
    )
    near = [hop(r, 1) for r in rows]
    xs = {0: rows}
    b2, a4 = hop(rows[1], 2), None
    if plan.group == 8:
        a4 = hop(rows[0], 4)
    a2 = hop(rows[0], 2)
    xs[2] = [a2, b2]
    if plan.group == 8:
        b4 = hop(rows[1], 4)
        xs[4] = [a4, b4]
        xs[6] = [hop(a4, 2), hop(b2, 4)]
    weights = lax.all_to_all(cut.reshape(tall), "dp", 0, 0, tiled=True)
    far = [m for m in xs if m]
    weights, *got = lax.optimization_barrier((weights, *(h for m in far for h in xs[m])))
    slots = [*rows, *near]
    for i in range(0, len(got), 2):
        slots += got[i : i + 2] + [hop(h, 1) for h in got[i : i + 2]]
    x, hidden, outw, own, send, marks = call(
        functools.partial(forward_kernel, plan),
        (weights, *slots),
        [
            ((2 * plan.xrows, total), BF16),
            ((2 * plan.cols, total), BF16),
            ((plan.classes, plan.cols), F32),
            (dense, F32),
            (dense, F32),
            (dense[1:], F32),
        ],
        [pltpu.VMEM((plan.xrows, plan.cols), F32)],
        cost=4,
    )
    own = own + hop(send, 1)
    more = [hop(own, k) for k in range(2, plan.group, 2)]
    (grads,) = call(
        functools.partial(backward_kernel, plan),
        (own, weights, outw, x, hidden, marks, *more),
        [(tall, F32)],
        [
            pltpu.VMEM(dense, F32),
            pltpu.VMEM((plan.classes, total), F32),
            pltpu.VMEM((2 * plan.cols, total), BF16),
            pltpu.VMEM((plan.xrows, plan.cols), F32),
        ],
        cost=4,
    )
    got = lax.all_to_all(grads, "dp", 0, 0, tiled=True)
    scale = pool / plan.batch
    count = n * plan.batch
    spot = jnp.stack([me * params.shape[0], last])
    base, old = call(
        functools.partial(prepare_kernel, plan),
        (spot, params.reshape(flat), momentum.reshape(flat), noise_draws.reshape(flat)),
        [(flat, F32), (flat, F32)],
        [pltpu.VMEM(flat, F32), pltpu.VMEM(flat, F32), pltpu.SemaphoreType.DMA((3,))],
        smem=1,
        whole=3,
    )
    new_params, new_momentum, loss = call(
        functools.partial(update_kernel, plan, scale, count),
        (spot, got, base, old),
        [(flat, F32), (flat, F32), ((1, LANES), F32)],
        [pltpu.VMEM(flat, F32)],
        smem=1,
    )
    return new_params.reshape(-1), new_momentum.reshape(-1), loss[0, :1]


def total_nll(flat_vec, din, chosen_rows, targets):
    in_end = din * H
    hid_end = in_end + H
    w_in = flat_vec[:in_end].reshape(din, H)
    b_in = flat_vec[in_end:hid_end]
    w_out = flat_vec[hid_end : hid_end + H * OUT].reshape(H, OUT)
    b_out = flat_vec[hid_end + H * OUT : hid_end + H * OUT + OUT]
    high = dict(precision=lax.Precision.HIGHEST, preferred_element_type=F32)
    hidden = jnp.tanh(jnp.dot(chosen_rows, w_in, **high) + b_in)
    logits = jnp.dot(hidden, w_out, **high) + b_out
    log_norm = jnp.log(jnp.sum(jnp.exp(logits), axis=1))
    classes = iota(logits.shape, 1)
    picked = jnp.sum(jnp.where(targets[:, None] == classes, logits, 0.0), axis=1)
    return jnp.sum(log_norm - picked)


def plain_body(params, momentum, noise_draws, images, labels, indices):
    shard_len = params.shape[0]
    din = images.shape[1]
    shard_start = lax.axis_index("dp") * shard_len
    precision = precision_of(shard_start + lax.iota(jnp.int32, shard_len), din)
    gathered = lax.all_gather(params, "dp", axis=0, tiled=True)
    chosen_rows = jnp.take(images, indices[0], axis=0)
    targets = jnp.take(labels, indices[0], axis=0)
    nll, pullback = jax.vjp(lambda w: total_nll(w, din, chosen_rows, targets), gathered)
    (local_grad,) = pullback(jnp.ones_like(nll))
    loss = lax.psum(nll, "dp") / (lax.axis_size("dp") * indices.shape[1])
    own_grad = lax.psum_scatter(local_grad, "dp", scatter_dimension=0, tiled=True)
    force = images.shape[0] / indices.shape[1] * own_grad + precision * params
    momentum = (1.0 - step_size * friction) * momentum - step_size * force
    momentum = momentum + math.sqrt(2.0 * friction * step_size) * noise_draws[0]
    return params + step_size * momentum, momentum, loss.reshape(1)


def solution(mesh):
    n = mesh.shape["dp"]

    def body(*args):
        params, images, indices = args[0], args[3], args[5]
        if Plan.fits(n, images.shape[1], params.shape[0], indices.shape[1]):
            return fast_body(n, *args)
        return plain_body(*args)

    placed = (
        P(("grp", "dp")),
        P(("grp", "dp")),
        P("grp", "dp"),
        P(("grp", "dp"), None),
        P(("grp", "dp")),
        P("grp", "dp"),
    )
    return jax.shard_map(
        body,
        mesh=mesh,
        in_specs=placed,
        out_specs=(P(("grp", "dp")), P(("grp", "dp")), P("grp")),
        check_vma=False,
    )
```

```python
import functools
import math

import jax
import jax.numpy as jnp
from jax import lax
from jax.experimental import pallas as pl
from jax.experimental.pallas import tpu as pltpu
from jax.sharding import PartitionSpec as P


H = 2048
OUT = 10
LANES = 128
SHARE = 0.62
COPIES = 2

step_size = 0.02
friction = 15.0
F32, BF16 = jnp.float32, jnp.bfloat16


def up8(n):
    return -(-n // 8) * 8


class Plan:
    def __init__(self, devices, din, shard_len, batch):
        self.n = devices
        self.group = devices // COPIES
        self.din = din
        self.cols = H // self.group
        self.nb = self.cols // LANES
        self.rows = shard_len // H
        self.pad = up8(self.rows + 1)
        self.step = H // LANES
        self.early, self.rest = (0, 2, 4), (1, 3, 5, 6, 7)
        self.flat = shard_len // LANES
        self.batch = batch
        self.tail = din + 1 - (devices - 1) * self.rows
        gcd = math.gcd(LANES, OUT)
        self.hp, self.qp = LANES // gcd, OUT // gcd
        self.periods = self.cols // self.hp
        self.classes = up8(OUT)
        self.xrows = -(-(din + 2) // 16) * 16
        first = round(SHARE * self.xrows / 16) * 16
        self.parts = (slice(0, first), slice(first, self.xrows))

    @staticmethod
    def fits(devices, din, shard_len, batch):
        if devices & (devices - 1) or devices < 2 * COPIES or shard_len % (8 * LANES) or shard_len % H:
            return False
        group, rows = devices // COPIES, shard_len // H
        if H % (group * LANES) or batch % LANES or group != 8 or din % 8:
            return False
        tail = din + 1 - (devices - 1) * rows
        return 0 < tail and tail + OUT + 1 <= rows


def split(x):
    hi = x.astype(BF16)
    return hi, (x - hi.astype(F32)).astype(BF16)


def split3(x):
    hi = x.astype(BF16)
    rest = x - hi.astype(F32)
    mid = rest.astype(BF16)
    return hi, mid, (rest - mid.astype(F32)).astype(BF16)


def dot(a, b, dims):
    return lax.dot_general(a, b, (dims, ((), ())), preferred_element_type=F32)


NN, NT = ((1,), (0,)), ((1,), (1,))


def iota(shape, axis):
    return lax.broadcasted_iota(jnp.int32, shape, axis)


def pick_kernel(plan, img_ref, meta_ref, *parts):
    pool = img_ref.shape[1]
    picks = meta_ref[:, pool:].astype(jnp.int32)
    hot = (iota((pool, plan.batch), 0) == picks).astype(BF16)
    hi, mid, lo = split3(img_ref[...])
    rows = dot(hi, hot, NN) + dot(mid, hot, NN) + dot(lo, hot, NN)
    spare = plan.xrows - plan.din
    marks = jnp.broadcast_to(meta_ref[:, :pool], (spare, pool)).astype(BF16)
    marks = dot(marks, hot, NN)
    at = iota((spare, plan.batch), 0)
    rows = jnp.concatenate([rows, jnp.where(at == 0, 1.0, jnp.where(at == 1, marks, 0.0))], axis=0)
    for part, ref in zip(plan.parts, parts):
        ref[...] = rows[part]


def cut_kernel(plan, last_ref, par_ref, out_ref):
    cut_weights(plan, last_ref, par_ref, out_ref)


def cut_weights(plan, last_ref, par_ref, out_ref):
    out_ref[...] = jnp.zeros_like(out_ref)
    for j in range(plan.group):
        for b in range(plan.nb):
            piece = par_ref[pl.ds(j * plan.nb + b, plan.rows, stride=plan.step), :]
            for d in range(j, plan.n, plan.group):
                out_ref[d, : plan.rows, b * LANES : (b + 1) * LANES] = piece

    @pl.when(last_ref[0] == 1)
    def _():
        t = plan.tail
        for j in range(plan.group):
            for d in range(j, plan.n, plan.group):
                out_ref[d, t + OUT, :LANES] = par_ref[(t + OUT) * plan.step, :]
            for b in range(plan.nb):
                start = t * plan.step + j * plan.nb * OUT + b
                piece = par_ref[pl.ds(start, OUT, stride=plan.nb), :]
                for d in range(j, plan.n, plan.group):
                    out_ref[d, t : t + OUT, b * LANES : (b + 1) * LANES] = piece


def class_masks(plan):
    width = plan.qp * LANES
    mask = (iota((plan.classes, width), 1) % OUT == iota((plan.classes, width), 0)).astype(F32)
    place = (iota((width, plan.hp), 0) // OUT == iota((width, plan.hp), 1)).astype(BF16)
    return mask, place


def flat_spot(plan, r):
    row = (plan.n - 1) * plan.pad + plan.tail + r // plan.nb
    col = r % plan.nb * LANES
    return row, col


def blocks_of(plan):
    return [(d, d * plan.rows, min(plan.rows, plan.din + 1 - d * plan.rows)) for d in range(plan.n)]


def out_weights(plan, w_ref, a_ref):
    mask, place = class_masks(plan)
    lhs = []
    for p in range(plan.periods):
        parts = []
        for q in range(plan.qp):
            row, col = flat_spot(plan, p * plan.qp + q)
            parts.append(jnp.broadcast_to(w_ref[row : row + 1, col : col + LANES], (plan.classes, LANES)))
        lhs.append(jnp.concatenate(parts, axis=1) * mask)
    hi, mid, lo = split3(jnp.concatenate(lhs, axis=0))
    out_w = dot(hi, place, NN) + dot(mid, place, NN) + dot(lo, place, NN)
    for p in range(plan.periods):
        rows = slice(p * plan.classes, (p + 1) * plan.classes)
        a_ref[:, p * plan.hp : (p + 1) * plan.hp] = out_w[rows]


def split_rows(plan, parts, x_ref, here):
    for part, ref in zip(plan.parts, parts):
        hi, lo = split(ref[...])
        x_ref[part, here] = hi
        x_ref[plan.xrows + part.start : plan.xrows + part.stop, here] = lo


def keep_labels(plan, m, ref, lab_ref):
    per = plan.batch // LANES
    mark = plan.din + 1 - plan.parts[1].start
    for i in range(per):
        row = ref[mark : mark + 1, i * LANES : (i + 1) * LANES]
        lab_ref[m * per + i : m * per + i + 1, :] = row


def forward_slot(plan, m, x, w_cat, a_cat, h_ref, here, own_ref, send_ref):
    per = plan.batch // LANES
    x_hi, x_lo = x
    pre = dot(w_cat, x_hi, NN)
    hidden = jnp.tanh(pre[: plan.cols] + (pre[plan.cols :] + dot(w_cat[: plan.cols], x_lo, NN)))
    h_hi, h_lo = split(hidden)
    h_ref[: plan.cols, here] = h_hi
    h_ref[plan.cols :, here] = h_lo
    lg = dot(a_cat, h_hi, NN)
    lg = lg[: plan.classes] + (lg[plan.classes :] + dot(a_cat[: plan.classes], h_lo, NN))
    for i in range(per):
        own, other = m * per + i, (m ^ 1) * per + i
        for o in range(OUT):
            row = lg[o : o + 1, i * LANES : (i + 1) * LANES]
            own_ref[o, own : own + 1, :] = row
            send_ref[o, other : other + 1, :] = row


def ready_kernel(plan, *refs):
    join_ref, lab_ref = refs[-2:]
    lab_ref[...] = jnp.zeros_like(lab_ref)
    for s, m in enumerate(plan.early):
        pair = refs[2 * s : 2 * s + 2]
        keep_labels(plan, m, pair[1], lab_ref)
        for part, ref in zip(plan.parts, pair):
            join_ref[s, part, :] = ref[...]


def front_kernel(plan, w_ref, join_ref, x_ref, h_ref, a_ref, cat_ref, own_ref, send_ref, c_ref):
    out_weights(plan, w_ref, a_ref)
    a_cat = jnp.concatenate(split(a_ref[...]), axis=0)
    c_ref[...] = jnp.zeros_like(c_ref)
    for d, first, rows in blocks_of(plan):
        c_ref[first : first + rows, :] = w_ref[d * plan.pad : d * plan.pad + rows, :]
    w_cat = jnp.concatenate(split(c_ref[...].T), axis=0)
    cat_ref[...] = w_cat
    own_ref[...] = jnp.zeros_like(own_ref)
    send_ref[...] = jnp.zeros_like(send_ref)
    for s, m in enumerate(plan.early):
        here = slice(s * plan.batch, (s + 1) * plan.batch)
        x = split(join_ref[s])
        x_ref[: plan.xrows, here] = x[0]
        x_ref[plan.xrows :, here] = x[1]
        forward_slot(plan, m, x, w_cat, a_cat, h_ref, here, own_ref, send_ref)


def rest_kernel(plan, cat_ref, a_ref, own1_ref, send1_ref, lab1_ref, join_ref, *refs):
    x_ref, h_ref, own_ref, send_ref, lab_ref = refs[-5:]
    own_ref[...] = own1_ref[...]
    send_ref[...] = send1_ref[...]
    lab_ref[...] = lab1_ref[...]
    w_cat = cat_ref[...]
    a_cat = jnp.concatenate(split(a_ref[...]), axis=0)
    mark, joined = plan.parts[1].start, len(plan.early)
    for s, m in enumerate(plan.rest):
        here = slice(s * plan.batch, (s + 1) * plan.batch)
        if s < joined:
            keep_labels(plan, m, join_ref.at[s, mark:, :], lab_ref)
            x = split(join_ref[s])
            x_ref[: plan.xrows, here] = x[0]
            x_ref[plan.xrows :, here] = x[1]
        else:
            pair = refs[2 * (s - joined) :][:2]
            keep_labels(plan, m, pair[1], lab_ref)
            split_rows(plan, pair, x_ref, here)
            x = x_ref[: plan.xrows, here], x_ref[plan.xrows :, here]
        forward_slot(plan, m, x, w_cat, a_cat, h_ref, here, own_ref, send_ref)


def backward_kernel(plan, own_ref, w_ref, a_ref, x1_ref, x2_ref, h1_ref, h2_ref, lab_ref, *refs):
    lg_refs, (out_ref, lg_ref, dl_ref, dh_ref, dw_ref) = refs[:-5], refs[-5:]
    per = plan.batch // LANES
    lines = plan.group * per
    order = (*plan.early, *plan.rest)
    diag = iota((plan.classes, LANES), 0) == iota((plan.classes, LANES), 1)
    row = (plan.n - 1) * plan.pad + plan.tail + OUT
    bias = w_ref[row : row + 1, :LANES]
    for m in range(plan.group):
        value = own_ref[:, m * per : (m + 1) * per, :]
        for i, ref in enumerate(lg_refs):
            other = m ^ (2 * (i + 1))
            value = value + ref[:, other * per : (other + 1) * per, :]
        lg_ref[:, m * per : (m + 1) * per, :] = value
    labels = lab_ref[...].astype(jnp.int32)
    logits = [lg_ref[o] + bias[:, o : o + 1] for o in range(OUT)]
    top = functools.reduce(jnp.maximum, logits)
    ex = [jnp.exp(v - top) for v in logits]
    norm = functools.reduce(jnp.add, ex)
    hits = [labels == o for o in range(OUT)]
    picked = functools.reduce(jnp.add, [jnp.where(h, v, 0.0) for h, v in zip(hits, logits)])
    nll = jnp.sum(jnp.sum(jnp.log(norm) + top - picked, axis=1, keepdims=True), axis=0, keepdims=True)
    share = 1.0 / norm
    dl_ref[...] = jnp.zeros_like(dl_ref)
    for o in range(OUT):
        value = ex[o] * share - jnp.where(hits[o], 1.0, 0.0)
        for i in range(lines):
            at = (order.index(i // per) * per + i % per) * LANES
            dl_ref[o : o + 1, at : at + LANES] = value[i : i + 1, :]
    dl = dl_ref[...]
    dbias = jnp.sum(dl, axis=1, keepdims=True)
    dbias = jnp.sum(jnp.where(diag, dbias, 0.0), axis=0, keepdims=True)
    dl_hi, dl_lo = split(dl)
    dl_cat = jnp.concatenate([dl_hi, dl_lo], axis=0)
    dl_three = jnp.concatenate([dl_hi, dl_hi, dl_lo], axis=0)
    a_hi, a_lo = split(a_ref[...])
    a_three = jnp.concatenate([v.astype(F32) for v in (a_hi, a_lo, a_hi)], axis=0).T.astype(BF16)
    cols, xrows, classes = plan.cols, plan.xrows, plan.classes
    da, start = 0.0, 0
    for h_ref in (h1_ref, h2_ref):
        width = h_ref.shape[1]
        for at in range(0, width, plan.batch):
            here = slice(start + at, start + at + plan.batch)
            local = slice(at, at + plan.batch)
            hidden = h_ref[:cols, local].astype(F32) + h_ref[cols:, local].astype(F32)
            dh = dot(a_three, dl_three[:, here], NN)
            dh_hi, dh_lo = split(dh * (1.0 - hidden * hidden))
            dh_ref[:cols, here] = dh_hi
            dh_ref[cols:, here] = dh_lo
        da = da + dot(h_ref[...], dl_cat[:, start : start + width], NT)
        start += width
    da = da.T
    da = da[:classes, :cols] + (da[classes:, :cols] + da[:classes, cols:])
    dw, start = 0.0, 0
    for x_ref in (x1_ref, x2_ref):
        here = slice(start, start + x_ref.shape[1])
        part = dot(x_ref[...], dh_ref[:cols, here], NT)
        dw = dw + (part[:xrows] + (part[xrows:] + dot(x_ref[:xrows, :], dh_ref[cols:, here], NT)))
        start = here.stop
    dw_ref[...] = dw
    out_ref[...] = jnp.zeros_like(out_ref)
    for d, first, count in blocks_of(plan):
        out_ref[d * plan.pad : d * plan.pad + count, :] = dw_ref[first : first + count, :]
    mask, place = class_masks(plan)
    hi, mid, lo = split3(da)
    parts = []
    for v in (hi, mid, lo):
        parts.append(jnp.concatenate([v[:, p * plan.hp : (p + 1) * plan.hp] for p in range(plan.periods)], axis=0))
    back = dot(parts[0], place, NT) + dot(parts[1], place, NT) + dot(parts[2], place, NT)
    for p in range(plan.periods):
        line = jnp.sum(back[p * plan.classes : (p + 1) * plan.classes] * mask, axis=0, keepdims=True)
        for q in range(plan.qp):
            r, c = flat_spot(plan, p * plan.qp + q)
            out_ref[r : r + 1, c : c + LANES] = line[:, q * LANES : (q + 1) * LANES]
    out_ref[row : row + 1, :LANES] = dbias
    for d in range(plan.n):
        at = d * plan.pad + plan.rows
        out_ref[at : at + 1, :LANES] = jnp.broadcast_to(nll, (1, LANES))


def prepare_kernel(plan, at_ref, par_ref, mom_ref, noise_ref, base_ref, keep_ref, mom, noise, sems):
    loads = [pltpu.make_async_copy(s, d, sems.at[i]) for i, (s, d) in enumerate(
        ((par_ref, keep_ref), (mom_ref, mom), (noise_ref, noise)))]
    for load in loads:
        load.start()
    for load in loads:
        load.wait()
    shape = (plan.flat, LANES)
    index = at_ref[0] + iota(shape, 0) * LANES + iota(shape, 1)
    prior = precision_of(index, plan.din) * keep_ref[...]
    base = (1.0 - step_size * friction) * mom[...] - step_size * prior
    base_ref[...] = base + math.sqrt(2.0 * friction * step_size) * noise[...]


def update_kernel(plan, scale, count, at_ref, got_ref, base_ref, par_ref, par_out, mom_out, loss_ref, grad_ref):
    t = plan.tail
    pieces = []
    for j in range(plan.group):
        piece = got_ref[j * plan.pad : (j + 1) * plan.pad, :]
        for g in range(1, COPIES):
            at = (g * plan.group + j) * plan.pad
            piece = piece + got_ref[at : at + plan.pad, :]
        pieces.append(piece)
        for b in range(plan.nb):
            lanes = slice(b * LANES, (b + 1) * LANES)
            grad_ref[pl.ds(j * plan.nb + b, plan.rows, stride=plan.step), :] = piece[: plan.rows, lanes]
    loss_ref[...] = pieces[0][plan.rows : plan.rows + 1, :LANES] * (1.0 / count)

    @pl.when(at_ref[1] == 1)
    def _():
        row = (t + OUT) * plan.step
        grad_ref[row:, :] = jnp.zeros((plan.flat - row, LANES), F32)
        grad_ref[row : row + 1, :] = pieces[0][t + OUT : t + OUT + 1, :LANES]
        for j in range(plan.group):
            for b in range(plan.nb):
                lanes = slice(b * LANES, (b + 1) * LANES)
                start = t * plan.step + j * plan.nb * OUT + b
                grad_ref[pl.ds(start, OUT, stride=plan.nb), :] = pieces[j][t : t + OUT, lanes]

    mom = base_ref[...] - (step_size * scale) * grad_ref[...]
    mom_out[...] = mom
    par_out[...] = par_ref[...] + step_size * mom


def precision_of(index, din):
    in_end = din * H
    hid_end = in_end + H
    out_end = hid_end + H * OUT
    inner = jnp.where(index < hid_end, 1.0, jnp.where(index < out_end, float(H), 1.0))
    return jnp.where(index < in_end, float(din), inner)


def call(kernel, args, outs, scratch=(), smem=0, limit=16, whole=0, cost=1):
    vm = pl.BlockSpec(memory_space=pltpu.VMEM)
    sm = pl.BlockSpec(memory_space=pltpu.SMEM)
    anywhere = pl.BlockSpec(memory_space=pltpu.HBM)
    specs = [sm] * smem + [anywhere] * whole
    return pl.pallas_call(
        kernel,
        out_shape=[jax.ShapeDtypeStruct(s, t) for s, t in outs],
        in_specs=specs + [vm] * (len(args) - len(specs)),
        out_specs=[vm] * len(outs),
        scratch_shapes=list(scratch),
        compiler_params=pltpu.CompilerParams(vmem_limit_bytes=limit << 20),
        cost_estimate=pl.CostEstimate(flops=cost * 10**9, bytes_accessed=1 << 20, transcendentals=0),
    )(*args)


def fast_body(n, params, momentum, noise_draws, images, labels, indices):
    pool, din = images.shape
    plan = Plan(n, din, params.shape[0], indices.shape[1])
    me = lax.axis_index("dp")
    last = (me == n - 1).astype(jnp.int32)
    flat = (plan.flat, LANES)
    tall = (n * plan.pad, plan.cols)
    total = plan.group * plan.batch
    dense = (OUT, total // LANES, LANES)

    def hop(x, k):
        return lax.ppermute(x, "dp", [(d, d ^ k) for d in range(n)])


    meta = jnp.concatenate([labels, indices[0]]).astype(F32).reshape(1, -1)
    a, b = call(
        functools.partial(pick_kernel, plan),
        (images.T, meta),
        [((part.stop - part.start, plan.batch), F32) for part in plan.parts],
    )
    b2 = hop(b, 2)
    a4 = hop(a, 4)
    a2 = hop(a, 2)
    b4 = hop(b, 4)
    a6 = hop(a4, 2)
    b6 = hop(b2, 4)
    (cut,) = call(
        functools.partial(cut_kernel, plan),
        (last.reshape(1), params.reshape(flat)),
        [((n, plan.pad, plan.cols), F32)],
        smem=1,
    )
    weights = lax.all_to_all(cut.reshape(tall), "dp", 0, 0, tiled=True)
    half = len(plan.early) * plan.batch
    join, marks = call(
        functools.partial(ready_kernel, plan),
        (a, b, a2, b2, a4, b4),
        [((len(plan.early), plan.xrows, plan.batch), F32), (dense[1:], F32)],
    )
    weights, join = lax.optimization_barrier((weights, join))
    other = hop(join, 1)
    x1, h1, outw, cat, own, send = call(
        functools.partial(front_kernel, plan),
        (weights, join),
        [
            ((2 * plan.xrows, half), BF16),
            ((2 * plan.cols, half), BF16),
            ((plan.classes, plan.cols), F32),
            ((2 * plan.cols, plan.xrows), BF16),
            (dense, F32),
            (dense, F32),
        ],
        [pltpu.VMEM((plan.xrows, plan.cols), F32)],
        cost=3,
    )
    outw, a6, b6 = lax.optimization_barrier((outw, a6, b6))
    x2, h2, own, send, marks = call(
        functools.partial(rest_kernel, plan),
        (cat, outw, own, send, marks, other, a6, b6, hop(a6, 1), hop(b6, 1)),
        [
            ((2 * plan.xrows, total - half), BF16),
            ((2 * plan.cols, total - half), BF16),
            (dense, F32),
            (dense, F32),
            (dense[1:], F32),
        ],
        cost=3,
    )
    own = own + hop(send, 1)
    more = [hop(own, k) for k in range(2, plan.group, 2)]
    (grads,) = call(
        functools.partial(backward_kernel, plan),
        (own, weights, outw, x1, x2, h1, h2, marks, *more),
        [(tall, F32)],
        [
            pltpu.VMEM(dense, F32),
            pltpu.VMEM((plan.classes, total), F32),
            pltpu.VMEM((2 * plan.cols, total), BF16),
            pltpu.VMEM((plan.xrows, plan.cols), F32),
        ],
        cost=4,
    )
    got = lax.all_to_all(grads, "dp", 0, 0, tiled=True)
    scale = pool / plan.batch
    count = n * plan.batch
    spot = jnp.stack([me * params.shape[0], last])
    base, old = call(
        functools.partial(prepare_kernel, plan),
        (spot, params.reshape(flat), momentum.reshape(flat), noise_draws.reshape(flat)),
        [(flat, F32), (flat, F32)],
        [pltpu.VMEM(flat, F32), pltpu.VMEM(flat, F32), pltpu.SemaphoreType.DMA((3,))],
        smem=1,
        whole=3,
    )
    new_params, new_momentum, loss = call(
        functools.partial(update_kernel, plan, scale, count),
        (spot, got, base, old),
        [(flat, F32), (flat, F32), ((1, LANES), F32)],
        [pltpu.VMEM(flat, F32)],
        smem=1,
    )
    return new_params.reshape(-1), new_momentum.reshape(-1), loss[0, :1]


def total_nll(flat_vec, din, chosen_rows, targets):
    in_end = din * H
    hid_end = in_end + H
    w_in = flat_vec[:in_end].reshape(din, H)
    b_in = flat_vec[in_end:hid_end]
    w_out = flat_vec[hid_end : hid_end + H * OUT].reshape(H, OUT)
    b_out = flat_vec[hid_end + H * OUT : hid_end + H * OUT + OUT]
    high = dict(precision=lax.Precision.HIGHEST, preferred_element_type=F32)
    hidden = jnp.tanh(jnp.dot(chosen_rows, w_in, **high) + b_in)
    logits = jnp.dot(hidden, w_out, **high) + b_out
    log_norm = jnp.log(jnp.sum(jnp.exp(logits), axis=1))
    classes = iota(logits.shape, 1)
    picked = jnp.sum(jnp.where(targets[:, None] == classes, logits, 0.0), axis=1)
    return jnp.sum(log_norm - picked)


def plain_body(params, momentum, noise_draws, images, labels, indices):
    shard_len = params.shape[0]
    din = images.shape[1]
    shard_start = lax.axis_index("dp") * shard_len
    precision = precision_of(shard_start + lax.iota(jnp.int32, shard_len), din)
    gathered = lax.all_gather(params, "dp", axis=0, tiled=True)
    chosen_rows = jnp.take(images, indices[0], axis=0)
    targets = jnp.take(labels, indices[0], axis=0)
    nll, pullback = jax.vjp(lambda w: total_nll(w, din, chosen_rows, targets), gathered)
    (local_grad,) = pullback(jnp.ones_like(nll))
    loss = lax.psum(nll, "dp") / (lax.axis_size("dp") * indices.shape[1])
    own_grad = lax.psum_scatter(local_grad, "dp", scatter_dimension=0, tiled=True)
    force = images.shape[0] / indices.shape[1] * own_grad + precision * params
    momentum = (1.0 - step_size * friction) * momentum - step_size * force
    momentum = momentum + math.sqrt(2.0 * friction * step_size) * noise_draws[0]
    return params + step_size * momentum, momentum, loss.reshape(1)


def solution(mesh):
    n = mesh.shape["dp"]

    def body(*args):
        params, images, indices = args[0], args[3], args[5]
        if Plan.fits(n, images.shape[1], params.shape[0], indices.shape[1]):
            return fast_body(n, *args)
        return plain_body(*args)

    placed = (
        P(("grp", "dp")),
        P(("grp", "dp")),
        P("grp", "dp"),
        P(("grp", "dp"), None),
        P(("grp", "dp")),
        P("grp", "dp"),
    )
    return jax.shard_map(
        body,
        mesh=mesh,
        in_specs=placed,
        out_specs=(P(("grp", "dp")), P(("grp", "dp")), P("grp")),
        check_vma=False,
    )
```

```python
import functools
import math

import jax
import jax.numpy as jnp
from jax import lax
from jax.experimental import pallas as pl
from jax.experimental.pallas import tpu as pltpu
from jax.sharding import PartitionSpec as P


H = 2048
OUT = 10
LANES = 128
SHARE = 0.72
COPIES = 2

step_size = 0.02
friction = 15.0
F32, BF16 = jnp.float32, jnp.bfloat16


def up8(n):
    return -(-n // 8) * 8


class Plan:
    def __init__(self, devices, din, shard_len, batch):
        self.n = devices
        self.group = devices // COPIES
        self.din = din
        self.cols = H // self.group
        self.nb = self.cols // LANES
        self.rows = shard_len // H
        self.unit = self.rows * self.nb
        self.back = self.unit + self.nb
        self.step = H // LANES
        self.early, self.middle, self.rest = (0, 2), (1, 3, 4), (5, 6, 7)
        self.flat = shard_len // LANES
        self.batch = batch
        self.tail = din + 1 - (devices - 1) * self.rows
        gcd = math.gcd(LANES, OUT)
        self.hp, self.qp = LANES // gcd, OUT // gcd
        self.periods = self.cols // self.hp
        self.classes = up8(OUT)
        self.xrows = -(-(din + 2) // 16) * 16
        first = round(SHARE * self.xrows / 16) * 16
        self.parts = (slice(0, first), slice(first, self.xrows))

    @staticmethod
    def fits(devices, din, shard_len, batch):
        if devices & (devices - 1) or devices < 2 * COPIES or shard_len % (8 * LANES) or shard_len % H:
            return False
        group, rows = devices // COPIES, shard_len // H
        if H % (group * LANES) or batch % LANES or group != 8 or din % 8:
            return False
        tail = din + 1 - (devices - 1) * rows
        return 0 < tail and tail + OUT + 1 <= rows


def split(x):
    hi = x.astype(BF16)
    return hi, (x - hi.astype(F32)).astype(BF16)


def split3(x):
    hi = x.astype(BF16)
    rest = x - hi.astype(F32)
    mid = rest.astype(BF16)
    return hi, mid, (rest - mid.astype(F32)).astype(BF16)


def dot(a, b, dims):
    return lax.dot_general(a, b, (dims, ((), ())), preferred_element_type=F32)


NN, NT = ((1,), (0,)), ((1,), (1,))


def iota(shape, axis):
    return lax.broadcasted_iota(jnp.int32, shape, axis)


def pick_kernel(plan, img_ref, meta_ref, *parts):
    pool = img_ref.shape[1]
    picks = meta_ref[:, pool:].astype(jnp.int32)
    hot = (iota((pool, plan.batch), 0) == picks).astype(BF16)
    hi, mid, lo = split3(img_ref[...])
    rows = dot(hi, hot, NN) + dot(mid, hot, NN) + dot(lo, hot, NN)
    spare = plan.xrows - plan.din
    marks = jnp.broadcast_to(meta_ref[:, :pool], (spare, pool)).astype(BF16)
    marks = dot(marks, hot, NN)
    at = iota((spare, plan.batch), 0)
    rows = jnp.concatenate([rows, jnp.where(at == 0, 1.0, jnp.where(at == 1, marks, 0.0))], axis=0)
    for part, ref in zip(plan.parts, parts):
        ref[...] = rows[part]


def cut_kernel(plan, last_ref, par_ref, out_ref):
    cut_weights(plan, last_ref, par_ref, out_ref)


def cut_weights(plan, last_ref, par_ref, out_ref):
    for j in range(plan.group):
        for b in range(plan.nb):
            piece = par_ref[pl.ds(j * plan.nb + b, plan.rows, stride=plan.step), :]
            for d in range(j, plan.n, plan.group):
                out_ref[pl.ds(d * plan.unit + b, plan.rows, stride=plan.nb), :] = piece

    @pl.when(last_ref[0] == 1)
    def _():
        t, count = plan.tail, OUT * plan.nb
        bias = par_ref[(t + OUT) * plan.step : (t + OUT) * plan.step + 1, :]
        for j in range(plan.group):
            start = t * plan.step + j * count
            piece = par_ref[start : start + count, :]
            for d in range(j, plan.n, plan.group):
                at = d * plan.unit + t * plan.nb
                out_ref[at : at + count, :] = piece
                out_ref[at + count : at + count + 1, :] = bias


def class_masks(plan):
    width = plan.qp * LANES
    mask = (iota((plan.classes, width), 1) % OUT == iota((plan.classes, width), 0)).astype(F32)
    place = (iota((width, plan.hp), 0) // OUT == iota((width, plan.hp), 1)).astype(BF16)
    return mask, place


def blocks_of(plan):
    return [(d, d * plan.rows, min(plan.rows, plan.din + 1 - d * plan.rows)) for d in range(plan.n)]


def out_weights(plan, w_ref, a_ref):
    mask, place = class_masks(plan)
    lhs = []
    for p in range(plan.periods):
        parts = []
        for q in range(plan.qp):
            row = (plan.n - 1) * plan.unit + plan.tail * plan.nb + p * plan.qp + q
            parts.append(jnp.broadcast_to(w_ref[row : row + 1, :], (plan.classes, LANES)))
        lhs.append(jnp.concatenate(parts, axis=1) * mask)
    hi, mid, lo = split3(jnp.concatenate(lhs, axis=0))
    out_w = dot(hi, place, NN) + dot(mid, place, NN) + dot(lo, place, NN)
    for p in range(plan.periods):
        rows = slice(p * plan.classes, (p + 1) * plan.classes)
        a_ref[:, p * plan.hp : (p + 1) * plan.hp] = out_w[rows]


def split_rows(plan, parts, x_ref, here):
    for part, ref in zip(plan.parts, parts):
        hi, lo = split(ref[...])
        x_ref[part, here] = hi
        x_ref[plan.xrows + part.start : plan.xrows + part.stop, here] = lo


def keep_labels(plan, m, ref, lab_ref):
    per = plan.batch // LANES
    mark = plan.din + 1 - plan.parts[1].start
    for i in range(per):
        row = ref[mark : mark + 1, i * LANES : (i + 1) * LANES]
        lab_ref[m * per + i : m * per + i + 1, :] = row


def forward_slot(plan, m, x, w_cat, a_cat, h_ref, here, own_ref, send_ref):
    per = plan.batch // LANES
    x_hi, x_lo = x
    pre = dot(w_cat, x_hi, NN)
    hidden = jnp.tanh(pre[: plan.cols] + (pre[plan.cols :] + dot(w_cat[: plan.cols], x_lo, NN)))
    h_hi, h_lo = split(hidden)
    h_ref[: plan.cols, here] = h_hi
    h_ref[plan.cols :, here] = h_lo
    lg = dot(a_cat, h_hi, NN)
    lg = lg[: plan.classes] + (lg[plan.classes :] + dot(a_cat[: plan.classes], h_lo, NN))
    for i in range(per):
        own, other = m * per + i, (m ^ 1) * per + i
        for o in range(OUT):
            row = lg[o : o + 1, i * LANES : (i + 1) * LANES]
            own_ref[o, own : own + 1, :] = row
            send_ref[o, other : other + 1, :] = row


def ready_kernel(plan, *refs):
    join_ref, lab_ref = refs[-2:]
    lab_ref[...] = jnp.zeros_like(lab_ref)
    for s, m in enumerate(plan.early):
        pair = refs[2 * s : 2 * s + 2]
        keep_labels(plan, m, pair[1], lab_ref)
        for part, ref in zip(plan.parts, pair):
            join_ref[s, part, :] = ref[...]


def front_kernel(plan, w_ref, join_ref, x_ref, h_ref, a_ref, cat_ref, own_ref, send_ref, c_ref):
    out_weights(plan, w_ref, a_ref)
    a_cat = jnp.concatenate(split(a_ref[...]), axis=0)
    c_ref[...] = jnp.zeros_like(c_ref)
    for d, first, rows in blocks_of(plan):
        for b in range(plan.nb):
            piece = w_ref[pl.ds(d * plan.unit + b, rows, stride=plan.nb), :]
            c_ref[first : first + rows, b * LANES : (b + 1) * LANES] = piece
    w_cat = jnp.concatenate(split(c_ref[...].T), axis=0)
    cat_ref[...] = w_cat
    own_ref[...] = jnp.zeros_like(own_ref)
    send_ref[...] = jnp.zeros_like(send_ref)
    for s, m in enumerate(plan.early):
        here = slice(s * plan.batch, (s + 1) * plan.batch)
        x = split(join_ref[s])
        x_ref[: plan.xrows, here] = x[0]
        x_ref[plan.xrows :, here] = x[1]
        forward_slot(plan, m, x, w_cat, a_cat, h_ref, here, own_ref, send_ref)


def later_kernel(plan, slots, joined, cat_ref, a_ref, own1_ref, send1_ref, lab1_ref, *refs):
    x_ref, h_ref, own_ref, send_ref, lab_ref = refs[-5:]
    own_ref[...] = own1_ref[...]
    send_ref[...] = send1_ref[...]
    lab_ref[...] = lab1_ref[...]
    w_cat = cat_ref[...]
    a_cat = jnp.concatenate(split(a_ref[...]), axis=0)
    pairs = refs[min(joined, 1) : -5]
    for s, m in enumerate(slots):
        here = slice(s * plan.batch, (s + 1) * plan.batch)
        if s < joined:
            keep_labels(plan, m, refs[0].at[s, plan.parts[1].start :, :], lab_ref)
            x = split(refs[0][s])
            x_ref[: plan.xrows, here] = x[0]
            x_ref[plan.xrows :, here] = x[1]
        else:
            pair = pairs[2 * (s - joined) :][:2]
            keep_labels(plan, m, pair[1], lab_ref)
            split_rows(plan, pair, x_ref, here)
            x = x_ref[: plan.xrows, here], x_ref[plan.xrows :, here]
        forward_slot(plan, m, x, w_cat, a_cat, h_ref, here, own_ref, send_ref)


def backward_kernel(plan, own_ref, w_ref, a_ref, x1_ref, x2_ref, x3_ref, h1_ref, h2_ref, h3_ref, lab_ref, *refs):
    lg_refs, (out_ref, lg_ref, dl_ref, dh_ref, dw_ref) = refs[:-5], refs[-5:]
    per = plan.batch // LANES
    lines = plan.group * per
    order = (*plan.early, *plan.middle, *plan.rest)
    diag = iota((plan.classes, LANES), 0) == iota((plan.classes, LANES), 1)
    row = (plan.n - 1) * plan.unit + (plan.tail + OUT) * plan.nb
    bias = w_ref[row : row + 1, :]
    for m in range(plan.group):
        value = own_ref[:, m * per : (m + 1) * per, :]
        for i, ref in enumerate(lg_refs):
            other = m ^ (2 * (i + 1))
            value = value + ref[:, other * per : (other + 1) * per, :]
        lg_ref[:, m * per : (m + 1) * per, :] = value
    labels = lab_ref[...].astype(jnp.int32)
    logits = [lg_ref[o] + bias[:, o : o + 1] for o in range(OUT)]
    top = functools.reduce(jnp.maximum, logits)
    ex = [jnp.exp(v - top) for v in logits]
    norm = functools.reduce(jnp.add, ex)
    hits = [labels == o for o in range(OUT)]
    picked = functools.reduce(jnp.add, [jnp.where(h, v, 0.0) for h, v in zip(hits, logits)])
    nll = jnp.sum(jnp.sum(jnp.log(norm) + top - picked, axis=1, keepdims=True), axis=0, keepdims=True)
    share = 1.0 / norm
    dl_ref[...] = jnp.zeros_like(dl_ref)
    for o in range(OUT):
        value = ex[o] * share - jnp.where(hits[o], 1.0, 0.0)
        for i in range(lines):
            at = (order.index(i // per) * per + i % per) * LANES
            dl_ref[o : o + 1, at : at + LANES] = value[i : i + 1, :]
    dl = dl_ref[...]
    dbias = jnp.sum(dl, axis=1, keepdims=True)
    dbias = jnp.sum(jnp.where(diag, dbias, 0.0), axis=0, keepdims=True)
    dl_hi, dl_lo = split(dl)
    dl_cat = jnp.concatenate([dl_hi, dl_lo], axis=0)
    dl_three = jnp.concatenate([dl_hi, dl_hi, dl_lo], axis=0)
    a_hi, a_lo = split(a_ref[...])
    a_three = jnp.concatenate([v.astype(F32) for v in (a_hi, a_lo, a_hi)], axis=0).T.astype(BF16)
    cols, xrows, classes = plan.cols, plan.xrows, plan.classes
    da, start = 0.0, 0
    for h_ref in (h1_ref, h2_ref, h3_ref):
        width = h_ref.shape[1]
        for at in range(0, width, plan.batch):
            here = slice(start + at, start + at + plan.batch)
            local = slice(at, at + plan.batch)
            hidden = h_ref[:cols, local].astype(F32) + h_ref[cols:, local].astype(F32)
            dh = dot(a_three, dl_three[:, here], NN)
            dh_hi, dh_lo = split(dh * (1.0 - hidden * hidden))
            dh_ref[:cols, here] = dh_hi
            dh_ref[cols:, here] = dh_lo
        da = da + dot(h_ref[...], dl_cat[:, start : start + width], NT)
        start += width
    da = da.T
    da = da[:classes, :cols] + (da[classes:, :cols] + da[:classes, cols:])
    dw, start = 0.0, 0
    for x_ref in (x1_ref, x2_ref, x3_ref):
        here = slice(start, start + x_ref.shape[1])
        part = dot(x_ref[...], dh_ref[:cols, here], NT)
        dw = dw + (part[:xrows] + (part[xrows:] + dot(x_ref[:xrows, :], dh_ref[cols:, here], NT)))
        start = here.stop
    dw_ref[...] = dw
    out_ref[...] = jnp.zeros_like(out_ref)
    for d, first, count in blocks_of(plan):
        for b in range(plan.nb):
            piece = dw_ref[first : first + count, b * LANES : (b + 1) * LANES]
            out_ref[pl.ds(d * plan.back + b, count, stride=plan.nb), :] = piece
    mask, place = class_masks(plan)
    hi, mid, lo = split3(da)
    parts = []
    for v in (hi, mid, lo):
        parts.append(jnp.concatenate([v[:, p * plan.hp : (p + 1) * plan.hp] for p in range(plan.periods)], axis=0))
    back = dot(parts[0], place, NT) + dot(parts[1], place, NT) + dot(parts[2], place, NT)
    for p in range(plan.periods):
        line = jnp.sum(back[p * plan.classes : (p + 1) * plan.classes] * mask, axis=0, keepdims=True)
        for q in range(plan.qp):
            r = (plan.n - 1) * plan.back + plan.tail * plan.nb + p * plan.qp + q
            out_ref[r : r + 1, :] = line[:, q * LANES : (q + 1) * LANES]
    row = (plan.n - 1) * plan.back + (plan.tail + OUT) * plan.nb
    out_ref[row : row + 1, :] = dbias
    for d in range(plan.n):
        at = d * plan.back + plan.unit
        out_ref[at : at + 1, :] = jnp.broadcast_to(nll, (1, LANES))


def prepare_kernel(plan, at_ref, par_ref, mom_ref, noise_ref, base_ref, keep_ref, mom, noise, sems):
    loads = [pltpu.make_async_copy(s, d, sems.at[i]) for i, (s, d) in enumerate(
        ((par_ref, keep_ref), (mom_ref, mom), (noise_ref, noise)))]
    for load in loads:
        load.start()
    for load in loads:
        load.wait()
    shape = (plan.flat, LANES)
    index = at_ref[0] + iota(shape, 0) * LANES + iota(shape, 1)
    prior = precision_of(index, plan.din) * keep_ref[...]
    base = (1.0 - step_size * friction) * mom[...] - step_size * prior
    base_ref[...] = base + math.sqrt(2.0 * friction * step_size) * noise[...]


def update_kernel(plan, scale, count, at_ref, got_ref, base_ref, par_ref, par_out, mom_out, loss_ref, grad_ref):
    def summed(j, start, size, stride=1):
        total = 0.0
        for g in range(COPIES):
            at = (g * plan.group + j) * plan.back + start
            total = total + got_ref[pl.ds(at, size, stride=stride), :]
        return total

    for j in range(plan.group):
        for b in range(plan.nb):
            spot = pl.ds(j * plan.nb + b, plan.rows, stride=plan.step)
            grad_ref[spot, :] = summed(j, b, plan.rows, plan.nb)
    loss_ref[...] = summed(0, plan.unit, 1) * (1.0 / count)

    @pl.when(at_ref[1] == 1)
    def _():
        t, size = plan.tail, OUT * plan.nb
        row = (t + OUT) * plan.step
        grad_ref[row:, :] = jnp.zeros((plan.flat - row, LANES), F32)
        grad_ref[row : row + 1, :] = summed(0, (t + OUT) * plan.nb, 1)
        for j in range(plan.group):
            at = t * plan.step + j * size
            grad_ref[at : at + size, :] = summed(j, t * plan.nb, size)

    mom = base_ref[...] - (step_size * scale) * grad_ref[...]
    mom_out[...] = mom
    par_out[...] = par_ref[...] + step_size * mom


def precision_of(index, din):
    in_end = din * H
    hid_end = in_end + H
    out_end = hid_end + H * OUT
    inner = jnp.where(index < hid_end, 1.0, jnp.where(index < out_end, float(H), 1.0))
    return jnp.where(index < in_end, float(din), inner)


def call(kernel, args, outs, scratch=(), smem=0, limit=16, whole=0, cost=1):
    vm = pl.BlockSpec(memory_space=pltpu.VMEM)
    sm = pl.BlockSpec(memory_space=pltpu.SMEM)
    anywhere = pl.BlockSpec(memory_space=pltpu.HBM)
    specs = [sm] * smem + [anywhere] * whole
    return pl.pallas_call(
        kernel,
        out_shape=[jax.ShapeDtypeStruct(s, t) for s, t in outs],
        in_specs=specs + [vm] * (len(args) - len(specs)),
        out_specs=[vm] * len(outs),
        scratch_shapes=list(scratch),
        compiler_params=pltpu.CompilerParams(vmem_limit_bytes=limit << 20),
        cost_estimate=pl.CostEstimate(flops=cost * 10**9, bytes_accessed=1 << 20, transcendentals=0),
    )(*args)


def fast_body(n, params, momentum, noise_draws, images, labels, indices):
    pool, din = images.shape
    plan = Plan(n, din, params.shape[0], indices.shape[1])
    me = lax.axis_index("dp")
    last = (me == n - 1).astype(jnp.int32)
    flat = (plan.flat, LANES)

    def exchange(x):
        x = x.reshape(n, -1, plan.nb, LANES)
        return lax.all_to_all(x, "dp", 0, 0, tiled=True).reshape(-1, LANES)

    total = plan.group * plan.batch
    dense = (OUT, total // LANES, LANES)

    def hop(x, k):
        return lax.ppermute(x, "dp", [(d, d ^ k) for d in range(n)])


    meta = jnp.concatenate([labels, indices[0]]).astype(F32).reshape(1, -1)
    a, b = call(
        functools.partial(pick_kernel, plan),
        (images.T, meta),
        [((part.stop - part.start, plan.batch), F32) for part in plan.parts],
    )
    b2 = hop(b, 2)
    a4 = hop(a, 4)
    a2 = hop(a, 2)
    b4 = hop(b, 4)
    a6 = hop(a4, 2)
    b6 = hop(b2, 4)
    (cut,) = call(
        functools.partial(cut_kernel, plan),
        (last.reshape(1), params.reshape(flat)),
        [((n * plan.unit, LANES), F32)],
        smem=1,
    )
    weights = exchange(cut)
    half = len(plan.early) * plan.batch
    join, marks = call(
        functools.partial(ready_kernel, plan),
        (a, b, a2, b2),
        [((len(plan.early), plan.xrows, plan.batch), F32), (dense[1:], F32)],
    )
    weights, join = lax.optimization_barrier((weights, join))
    other = hop(join, 1)
    x1, h1, outw, cat, own, send = call(
        functools.partial(front_kernel, plan),
        (weights, join),
        [
            ((2 * plan.xrows, half), BF16),
            ((2 * plan.cols, half), BF16),
            ((plan.classes, plan.cols), F32),
            ((2 * plan.cols, plan.xrows), BF16),
            (dense, F32),
            (dense, F32),
        ],
        [pltpu.VMEM((plan.xrows, plan.cols), F32)],
        cost=3,
    )

    def later(slots, joined, *args):
        width = len(slots) * plan.batch
        return call(
            functools.partial(later_kernel, plan, slots, joined),
            (cat, outw, own, send, marks, *args),
            [
                ((2 * plan.xrows, width), BF16),
                ((2 * plan.cols, width), BF16),
                (dense, F32),
                (dense, F32),
                (dense[1:], F32),
            ],
            cost=2,
        )

    a5, b5 = hop(a4, 1), hop(b4, 1)
    outw, a6, b6 = lax.optimization_barrier((outw, a6, b6))
    a7, b7 = hop(a6, 1), hop(b6, 1)
    x2, h2, own, send, marks = later(plan.middle, len(plan.early), other, a4, b4)
    x3, h3, own, send, marks = later(plan.rest, 0, a5, b5, a6, b6, a7, b7)
    own = own + hop(send, 1)
    more = [hop(own, k) for k in range(2, plan.group, 2)]
    (grads,) = call(
        functools.partial(backward_kernel, plan),
        (own, weights, outw, x1, x2, x3, h1, h2, h3, marks, *more),
        [((n * plan.back, LANES), F32)],
        [
            pltpu.VMEM(dense, F32),
            pltpu.VMEM((plan.classes, total), F32),
            pltpu.VMEM((2 * plan.cols, total), BF16),
            pltpu.VMEM((plan.xrows, plan.cols), F32),
        ],
        cost=4,
    )
    got = exchange(grads)
    scale = pool / plan.batch
    count = n * plan.batch
    spot = jnp.stack([me * params.shape[0], last])
    base, old = call(
        functools.partial(prepare_kernel, plan),
        (spot, params.reshape(flat), momentum.reshape(flat), noise_draws.reshape(flat)),
        [(flat, F32), (flat, F32)],
        [pltpu.VMEM(flat, F32), pltpu.VMEM(flat, F32), pltpu.SemaphoreType.DMA((3,))],
        smem=1,
        whole=3,
    )
    new_params, new_momentum, loss = call(
        functools.partial(update_kernel, plan, scale, count),
        (spot, got, base, old),
        [(flat, F32), (flat, F32), ((1, LANES), F32)],
        [pltpu.VMEM(flat, F32)],
        smem=1,
    )
    return new_params.reshape(-1), new_momentum.reshape(-1), loss[0, :1]


def total_nll(flat_vec, din, chosen_rows, targets):
    in_end = din * H
    hid_end = in_end + H
    w_in = flat_vec[:in_end].reshape(din, H)
    b_in = flat_vec[in_end:hid_end]
    w_out = flat_vec[hid_end : hid_end + H * OUT].reshape(H, OUT)
    b_out = flat_vec[hid_end + H * OUT : hid_end + H * OUT + OUT]
    high = dict(precision=lax.Precision.HIGHEST, preferred_element_type=F32)
    hidden = jnp.tanh(jnp.dot(chosen_rows, w_in, **high) + b_in)
    logits = jnp.dot(hidden, w_out, **high) + b_out
    log_norm = jnp.log(jnp.sum(jnp.exp(logits), axis=1))
    classes = iota(logits.shape, 1)
    picked = jnp.sum(jnp.where(targets[:, None] == classes, logits, 0.0), axis=1)
    return jnp.sum(log_norm - picked)


def plain_body(params, momentum, noise_draws, images, labels, indices):
    shard_len = params.shape[0]
    din = images.shape[1]
    shard_start = lax.axis_index("dp") * shard_len
    precision = precision_of(shard_start + lax.iota(jnp.int32, shard_len), din)
    gathered = lax.all_gather(params, "dp", axis=0, tiled=True)
    chosen_rows = jnp.take(images, indices[0], axis=0)
    targets = jnp.take(labels, indices[0], axis=0)
    nll, pullback = jax.vjp(lambda w: total_nll(w, din, chosen_rows, targets), gathered)
    (local_grad,) = pullback(jnp.ones_like(nll))
    loss = lax.psum(nll, "dp") / (lax.axis_size("dp") * indices.shape[1])
    own_grad = lax.psum_scatter(local_grad, "dp", scatter_dimension=0, tiled=True)
    force = images.shape[0] / indices.shape[1] * own_grad + precision * params
    momentum = (1.0 - step_size * friction) * momentum - step_size * force
    momentum = momentum + math.sqrt(2.0 * friction * step_size) * noise_draws[0]
    return params + step_size * momentum, momentum, loss.reshape(1)


def solution(mesh):
    n = mesh.shape["dp"]

    def body(*args):
        params, images, indices = args[0], args[3], args[5]
        if Plan.fits(n, images.shape[1], params.shape[0], indices.shape[1]):
            return fast_body(n, *args)
        return plain_body(*args)

    placed = (
        P(("grp", "dp")),
        P(("grp", "dp")),
        P("grp", "dp"),
        P(("grp", "dp"), None),
        P(("grp", "dp")),
        P("grp", "dp"),
    )
    return jax.shard_map(
        body,
        mesh=mesh,
        in_specs=placed,
        out_specs=(P(("grp", "dp")), P(("grp", "dp")), P("grp")),
        check_vma=False,
    )
```

```python
import functools
import math

import jax
import jax.numpy as jnp
from jax import lax
from jax.experimental import pallas as pl
from jax.experimental.pallas import tpu as pltpu
from jax.sharding import PartitionSpec as P


H = 2048
OUT = 10
LANES = 128
SHARE = 0.72
COPIES = 2

step_size = 0.02
friction = 15.0
F32, BF16 = jnp.float32, jnp.bfloat16


def up8(n):
    return -(-n // 8) * 8


class Plan:
    def __init__(self, devices, din, shard_len, batch):
        self.n = devices
        self.group = devices // COPIES
        self.din = din
        self.cols = H // self.group
        self.nb = self.cols // LANES
        self.rows = shard_len // H
        self.unit = self.rows * self.nb
        self.back = self.unit + self.nb
        self.step = H // LANES
        self.early, self.middle, self.rest = (0, 2), (1, 3, 4), (5, 6, 7)
        self.flat = shard_len // LANES
        self.batch = batch
        self.tail = din + 1 - (devices - 1) * self.rows
        gcd = math.gcd(LANES, OUT)
        self.hp, self.qp = LANES // gcd, OUT // gcd
        self.periods = self.cols // self.hp
        self.classes = up8(OUT)
        self.xrows = -(-(din + 2) // 16) * 16
        first = round(SHARE * self.xrows / 16) * 16
        self.parts = (slice(0, first), slice(first, self.xrows))

    @staticmethod
    def fits(devices, din, shard_len, batch):
        if devices & (devices - 1) or devices < 2 * COPIES or shard_len % (8 * LANES) or shard_len % H:
            return False
        group, rows = devices // COPIES, shard_len // H
        if H % (group * LANES) or batch % LANES or group != 8 or din % 8:
            return False
        tail = din + 1 - (devices - 1) * rows
        return 0 < tail and tail + OUT + 1 <= rows


def split(x):
    hi = x.astype(BF16)
    return hi, (x - hi.astype(F32)).astype(BF16)


def split3(x):
    hi = x.astype(BF16)
    rest = x - hi.astype(F32)
    mid = rest.astype(BF16)
    return hi, mid, (rest - mid.astype(F32)).astype(BF16)


def dot(a, b, dims):
    return lax.dot_general(a, b, (dims, ((), ())), preferred_element_type=F32)


NN, NT = ((1,), (0,)), ((1,), (1,))


def iota(shape, axis):
    return lax.broadcasted_iota(jnp.int32, shape, axis)


def pick_kernel(plan, img_ref, meta_ref, *parts):
    pool = img_ref.shape[1]
    picks = meta_ref[:, pool:].astype(jnp.int32)
    hot = (iota((pool, plan.batch), 0) == picks).astype(BF16)
    hi, mid, lo = split3(img_ref[...])
    rows = dot(hi, hot, NN) + dot(mid, hot, NN) + dot(lo, hot, NN)
    spare = plan.xrows - plan.din
    marks = jnp.broadcast_to(meta_ref[:, :pool], (spare, pool)).astype(BF16)
    marks = dot(marks, hot, NN)
    at = iota((spare, plan.batch), 0)
    rows = jnp.concatenate([rows, jnp.where(at == 0, 1.0, jnp.where(at == 1, marks, 0.0))], axis=0)
    for part, ref in zip(plan.parts, parts):
        ref[...] = rows[part]


def cut_kernel(plan, last_ref, par_ref, out_ref):
    cut_weights(plan, last_ref, par_ref, out_ref)


def cut_weights(plan, last_ref, par_ref, out_ref):
    for j in range(plan.group):
        for b in range(plan.nb):
            piece = par_ref[pl.ds(j * plan.nb + b, plan.rows, stride=plan.step), :]
            for d in range(j, plan.n, plan.group):
                out_ref[pl.ds(d * plan.unit + b, plan.rows, stride=plan.nb), :] = piece

    @pl.when(last_ref[0] == 1)
    def _():
        t, count = plan.tail, OUT * plan.nb
        bias = par_ref[(t + OUT) * plan.step : (t + OUT) * plan.step + 1, :]
        for j in range(plan.group):
            start = t * plan.step + j * count
            piece = par_ref[start : start + count, :]
            for d in range(j, plan.n, plan.group):
                at = d * plan.unit + t * plan.nb
                out_ref[at : at + count, :] = piece
                out_ref[at + count : at + count + 1, :] = bias


def class_masks(plan):
    width = plan.qp * LANES
    mask = (iota((plan.classes, width), 1) % OUT == iota((plan.classes, width), 0)).astype(F32)
    place = (iota((width, plan.hp), 0) // OUT == iota((width, plan.hp), 1)).astype(BF16)
    return mask, place


def blocks_of(plan):
    return [(d, d * plan.rows, min(plan.rows, plan.din + 1 - d * plan.rows)) for d in range(plan.n)]


def out_weights(plan, w_ref, a_ref):
    mask, place = class_masks(plan)
    lhs = []
    for p in range(plan.periods):
        parts = []
        for q in range(plan.qp):
            row = (plan.n - 1) * plan.unit + plan.tail * plan.nb + p * plan.qp + q
            parts.append(jnp.broadcast_to(w_ref[row : row + 1, :], (plan.classes, LANES)))
        lhs.append(jnp.concatenate(parts, axis=1) * mask)
    hi, mid, lo = split3(jnp.concatenate(lhs, axis=0))
    out_w = dot(hi, place, NN) + dot(mid, place, NN) + dot(lo, place, NN)
    for p in range(plan.periods):
        rows = slice(p * plan.classes, (p + 1) * plan.classes)
        a_ref[:, p * plan.hp : (p + 1) * plan.hp] = out_w[rows]


def split_rows(plan, parts, x_ref, here):
    for part, ref in zip(plan.parts, parts):
        hi, lo = split(ref[...])
        x_ref[part, here] = hi
        x_ref[plan.xrows + part.start : plan.xrows + part.stop, here] = lo


def keep_labels(plan, m, ref, lab_ref):
    per = plan.batch // LANES
    mark = plan.din + 1 - plan.parts[1].start
    for i in range(per):
        row = ref[mark : mark + 1, i * LANES : (i + 1) * LANES]
        lab_ref[m * per + i : m * per + i + 1, :] = row


def forward_slots(plan, slots, x_ref, w_cat, a_cat, h_ref, own_ref, send_ref):
    per = plan.batch // LANES
    pre = dot(w_cat, x_ref[: plan.xrows, :], NN)
    pre = pre[: plan.cols] + (pre[plan.cols :] + dot(w_cat[: plan.cols], x_ref[plan.xrows :, :], NN))
    h_hi, h_lo = split(jnp.tanh(pre))
    h_ref[: plan.cols, :] = h_hi
    h_ref[plan.cols :, :] = h_lo
    lg = dot(a_cat, h_hi, NN)
    lg = lg[: plan.classes] + (lg[plan.classes :] + dot(a_cat[: plan.classes], h_lo, NN))
    for s, m in enumerate(slots):
        for i in range(per):
            own, other, at = m * per + i, (m ^ 1) * per + i, (s * per + i) * LANES
            for o in range(OUT):
                row = lg[o : o + 1, at : at + LANES]
                own_ref[o, own : own + 1, :] = row
                send_ref[o, other : other + 1, :] = row


def ready_kernel(plan, *refs):
    join_ref, lab_ref = refs[-2:]
    lab_ref[...] = jnp.zeros_like(lab_ref)
    for s, m in enumerate(plan.early):
        pair = refs[2 * s : 2 * s + 2]
        keep_labels(plan, m, pair[1], lab_ref)
        for part, ref in zip(plan.parts, pair):
            join_ref[s, part, :] = ref[...]


def front_kernel(plan, w_ref, join_ref, x_ref, h_ref, a_ref, cat_ref, own_ref, send_ref, c_ref):
    out_weights(plan, w_ref, a_ref)
    a_cat = jnp.concatenate(split(a_ref[...]), axis=0)
    c_ref[...] = jnp.zeros_like(c_ref)
    for d, first, rows in blocks_of(plan):
        for b in range(plan.nb):
            piece = w_ref[pl.ds(d * plan.unit + b, rows, stride=plan.nb), :]
            c_ref[first : first + rows, b * LANES : (b + 1) * LANES] = piece
    w_cat = jnp.concatenate(split(c_ref[...].T), axis=0)
    cat_ref[...] = w_cat
    own_ref[...] = jnp.zeros_like(own_ref)
    send_ref[...] = jnp.zeros_like(send_ref)
    for s, m in enumerate(plan.early):
        here = slice(s * plan.batch, (s + 1) * plan.batch)
        x = split(join_ref[s])
        x_ref[: plan.xrows, here] = x[0]
        x_ref[plan.xrows :, here] = x[1]
    forward_slots(plan, plan.early, x_ref, w_cat, a_cat, h_ref, own_ref, send_ref)


def later_kernel(plan, slots, joined, cat_ref, a_ref, own1_ref, send1_ref, lab1_ref, *refs):
    x_ref, h_ref, own_ref, send_ref, lab_ref = refs[-5:]
    own_ref[...] = own1_ref[...]
    send_ref[...] = send1_ref[...]
    lab_ref[...] = lab1_ref[...]
    w_cat = cat_ref[...]
    a_cat = jnp.concatenate(split(a_ref[...]), axis=0)
    pairs = refs[min(joined, 1) : -5]
    for s, m in enumerate(slots):
        here = slice(s * plan.batch, (s + 1) * plan.batch)
        if s < joined:
            keep_labels(plan, m, refs[0].at[s, plan.parts[1].start :, :], lab_ref)
            x = split(refs[0][s])
            x_ref[: plan.xrows, here] = x[0]
            x_ref[plan.xrows :, here] = x[1]
        else:
            pair = pairs[2 * (s - joined) :][:2]
            keep_labels(plan, m, pair[1], lab_ref)
            split_rows(plan, pair, x_ref, here)
    forward_slots(plan, slots, x_ref, w_cat, a_cat, h_ref, own_ref, send_ref)


def backward_kernel(plan, own_ref, w_ref, a_ref, x1_ref, x2_ref, x3_ref, h1_ref, h2_ref, h3_ref, lab_ref, *refs):
    lg_refs, (out_ref, lg_ref, dl_ref, dh_ref, dw_ref) = refs[:-5], refs[-5:]
    per = plan.batch // LANES
    lines = plan.group * per
    order = (*plan.early, *plan.middle, *plan.rest)
    diag = iota((plan.classes, LANES), 0) == iota((plan.classes, LANES), 1)
    row = (plan.n - 1) * plan.unit + (plan.tail + OUT) * plan.nb
    bias = w_ref[row : row + 1, :]
    for m in range(plan.group):
        value = own_ref[:, m * per : (m + 1) * per, :]
        for i, ref in enumerate(lg_refs):
            other = m ^ (2 * (i + 1))
            value = value + ref[:, other * per : (other + 1) * per, :]
        lg_ref[:, m * per : (m + 1) * per, :] = value
    labels = lab_ref[...].astype(jnp.int32)
    logits = [lg_ref[o] + bias[:, o : o + 1] for o in range(OUT)]
    top = functools.reduce(jnp.maximum, logits)
    ex = [jnp.exp(v - top) for v in logits]
    norm = functools.reduce(jnp.add, ex)
    hits = [labels == o for o in range(OUT)]
    picked = functools.reduce(jnp.add, [jnp.where(h, v, 0.0) for h, v in zip(hits, logits)])
    nll = jnp.sum(jnp.sum(jnp.log(norm) + top - picked, axis=1, keepdims=True), axis=0, keepdims=True)
    share = 1.0 / norm
    dl_ref[...] = jnp.zeros_like(dl_ref)
    for o in range(OUT):
        value = ex[o] * share - jnp.where(hits[o], 1.0, 0.0)
        for i in range(lines):
            at = (order.index(i // per) * per + i % per) * LANES
            dl_ref[o : o + 1, at : at + LANES] = value[i : i + 1, :]
    dl = dl_ref[...]
    dbias = jnp.sum(dl, axis=1, keepdims=True)
    dbias = jnp.sum(jnp.where(diag, dbias, 0.0), axis=0, keepdims=True)
    dl_hi, dl_lo = split(dl)
    dl_cat = jnp.concatenate([dl_hi, dl_lo], axis=0)
    dl_three = jnp.concatenate([dl_hi, dl_hi, dl_lo], axis=0)
    a_hi, a_lo = split(a_ref[...])
    a_three = jnp.concatenate([v.astype(F32) for v in (a_hi, a_lo, a_hi)], axis=0).T.astype(BF16)
    cols, xrows, classes = plan.cols, plan.xrows, plan.classes
    da, start = 0.0, 0
    for h_ref in (h1_ref, h2_ref, h3_ref):
        width = h_ref.shape[1]
        for at in range(0, width, plan.batch):
            here = slice(start + at, start + at + plan.batch)
            local = slice(at, at + plan.batch)
            hidden = h_ref[:cols, local].astype(F32) + h_ref[cols:, local].astype(F32)
            dh = dot(a_three, dl_three[:, here], NN)
            dh_hi, dh_lo = split(dh * (1.0 - hidden * hidden))
            dh_ref[:cols, here] = dh_hi
            dh_ref[cols:, here] = dh_lo
        da = da + dot(h_ref[...], dl_cat[:, start : start + width], NT)
        start += width
    da = da.T
    da = da[:classes, :cols] + (da[classes:, :cols] + da[:classes, cols:])
    dw, start = 0.0, 0
    for x_ref in (x1_ref, x2_ref, x3_ref):
        here = slice(start, start + x_ref.shape[1])
        part = dot(x_ref[...], dh_ref[:cols, here], NT)
        dw = dw + (part[:xrows] + (part[xrows:] + dot(x_ref[:xrows, :], dh_ref[cols:, here], NT)))
        start = here.stop
    dw_ref[...] = dw
    out_ref[...] = jnp.zeros_like(out_ref)
    for d, first, count in blocks_of(plan):
        for b in range(plan.nb):
            piece = dw_ref[first : first + count, b * LANES : (b + 1) * LANES]
            out_ref[pl.ds(d * plan.back + b, count, stride=plan.nb), :] = piece
    mask, place = class_masks(plan)
    hi, mid, lo = split3(da)
    parts = []
    for v in (hi, mid, lo):
        parts.append(jnp.concatenate([v[:, p * plan.hp : (p + 1) * plan.hp] for p in range(plan.periods)], axis=0))
    back = dot(parts[0], place, NT) + dot(parts[1], place, NT) + dot(parts[2], place, NT)
    for p in range(plan.periods):
        line = jnp.sum(back[p * plan.classes : (p + 1) * plan.classes] * mask, axis=0, keepdims=True)
        for q in range(plan.qp):
            r = (plan.n - 1) * plan.back + plan.tail * plan.nb + p * plan.qp + q
            out_ref[r : r + 1, :] = line[:, q * LANES : (q + 1) * LANES]
    row = (plan.n - 1) * plan.back + (plan.tail + OUT) * plan.nb
    out_ref[row : row + 1, :] = dbias
    for d in range(plan.n):
        at = d * plan.back + plan.unit
        out_ref[at : at + 1, :] = jnp.broadcast_to(nll, (1, LANES))


def prepare_kernel(plan, at_ref, par_ref, mom_ref, noise_ref, base_ref, keep_ref, mom, noise, sems):
    loads = [pltpu.make_async_copy(s, d, sems.at[i]) for i, (s, d) in enumerate(
        ((par_ref, keep_ref), (mom_ref, mom), (noise_ref, noise)))]
    for load in loads:
        load.start()
    for load in loads:
        load.wait()
    shape = (plan.flat, LANES)
    index = at_ref[0] + iota(shape, 0) * LANES + iota(shape, 1)
    prior = precision_of(index, plan.din) * keep_ref[...]
    base = (1.0 - step_size * friction) * mom[...] - step_size * prior
    base_ref[...] = base + math.sqrt(2.0 * friction * step_size) * noise[...]


def update_kernel(plan, scale, count, at_ref, got_ref, base_ref, par_ref, par_out, mom_out, loss_ref, grad_ref):
    def summed(j, start, size, stride=1):
        total = 0.0
        for g in range(COPIES):
            at = (g * plan.group + j) * plan.back + start
            total = total + got_ref[pl.ds(at, size, stride=stride), :]
        return total

    for j in range(plan.group):
        for b in range(plan.nb):
            spot = pl.ds(j * plan.nb + b, plan.rows, stride=plan.step)
            grad_ref[spot, :] = summed(j, b, plan.rows, plan.nb)
    loss_ref[...] = summed(0, plan.unit, 1) * (1.0 / count)

    @pl.when(at_ref[1] == 1)
    def _():
        t, size = plan.tail, OUT * plan.nb
        row = (t + OUT) * plan.step
        grad_ref[row:, :] = jnp.zeros((plan.flat - row, LANES), F32)
        grad_ref[row : row + 1, :] = summed(0, (t + OUT) * plan.nb, 1)
        for j in range(plan.group):
            at = t * plan.step + j * size
            grad_ref[at : at + size, :] = summed(j, t * plan.nb, size)

    mom = base_ref[...] - (step_size * scale) * grad_ref[...]
    mom_out[...] = mom
    par_out[...] = par_ref[...] + step_size * mom


def precision_of(index, din):
    in_end = din * H
    hid_end = in_end + H
    out_end = hid_end + H * OUT
    inner = jnp.where(index < hid_end, 1.0, jnp.where(index < out_end, float(H), 1.0))
    return jnp.where(index < in_end, float(din), inner)


def call(kernel, args, outs, scratch=(), smem=0, limit=16, whole=0, cost=1):
    vm = pl.BlockSpec(memory_space=pltpu.VMEM)
    sm = pl.BlockSpec(memory_space=pltpu.SMEM)
    anywhere = pl.BlockSpec(memory_space=pltpu.HBM)
    specs = [sm] * smem + [anywhere] * whole
    return pl.pallas_call(
        kernel,
        out_shape=[jax.ShapeDtypeStruct(s, t) for s, t in outs],
        in_specs=specs + [vm] * (len(args) - len(specs)),
        out_specs=[vm] * len(outs),
        scratch_shapes=list(scratch),
        compiler_params=pltpu.CompilerParams(vmem_limit_bytes=limit << 20),
        cost_estimate=pl.CostEstimate(flops=cost * 10**9, bytes_accessed=1 << 20, transcendentals=0),
    )(*args)


def fast_body(n, params, momentum, noise_draws, images, labels, indices):
    pool, din = images.shape
    plan = Plan(n, din, params.shape[0], indices.shape[1])
    me = lax.axis_index("dp")
    last = (me == n - 1).astype(jnp.int32)
    flat = (plan.flat, LANES)

    def exchange(x):
        x = x.reshape(n, -1, plan.nb, LANES)
        return lax.all_to_all(x, "dp", 0, 0, tiled=True).reshape(-1, LANES)

    total = plan.group * plan.batch
    dense = (OUT, total // LANES, LANES)

    def hop(x, k):
        return lax.ppermute(x, "dp", [(d, d ^ k) for d in range(n)])


    meta = jnp.concatenate([labels, indices[0]]).astype(F32).reshape(1, -1)
    a, b = call(
        functools.partial(pick_kernel, plan),
        (images.T, meta),
        [((part.stop - part.start, plan.batch), F32) for part in plan.parts],
    )
    b2 = hop(b, 2)
    a4 = hop(a, 4)
    a2 = hop(a, 2)
    b4 = hop(b, 4)
    a6 = hop(a4, 2)
    b6 = hop(b2, 4)
    (cut,) = call(
        functools.partial(cut_kernel, plan),
        (last.reshape(1), params.reshape(flat)),
        [((n * plan.unit, LANES), F32)],
        smem=1,
    )
    weights = exchange(cut)
    half = len(plan.early) * plan.batch
    join, marks = call(
        functools.partial(ready_kernel, plan),
        (a, b, a2, b2),
        [((len(plan.early), plan.xrows, plan.batch), F32), (dense[1:], F32)],
    )
    weights, join = lax.optimization_barrier((weights, join))
    other = hop(join, 1)
    x1, h1, outw, cat, own, send = call(
        functools.partial(front_kernel, plan),
        (weights, join),
        [
            ((2 * plan.xrows, half), BF16),
            ((2 * plan.cols, half), BF16),
            ((plan.classes, plan.cols), F32),
            ((2 * plan.cols, plan.xrows), BF16),
            (dense, F32),
            (dense, F32),
        ],
        [pltpu.VMEM((plan.xrows, plan.cols), F32)],
        cost=3,
    )

    def later(slots, joined, *args):
        width = len(slots) * plan.batch
        return call(
            functools.partial(later_kernel, plan, slots, joined),
            (cat, outw, own, send, marks, *args),
            [
                ((2 * plan.xrows, width), BF16),
                ((2 * plan.cols, width), BF16),
                (dense, F32),
                (dense, F32),
                (dense[1:], F32),
            ],
            cost=2,
        )

    a5, b5 = hop(a4, 1), hop(b4, 1)
    outw, a6, b6 = lax.optimization_barrier((outw, a6, b6))
    a7, b7 = hop(a6, 1), hop(b6, 1)
    x2, h2, own, send, marks = later(plan.middle, len(plan.early), other, a4, b4)
    x3, h3, own, send, marks = later(plan.rest, 0, a5, b5, a6, b6, a7, b7)
    own = own + hop(send, 1)
    more = [hop(own, k) for k in range(2, plan.group, 2)]
    (grads,) = call(
        functools.partial(backward_kernel, plan),
        (own, weights, outw, x1, x2, x3, h1, h2, h3, marks, *more),
        [((n * plan.back, LANES), F32)],
        [
            pltpu.VMEM(dense, F32),
            pltpu.VMEM((plan.classes, total), F32),
            pltpu.VMEM((2 * plan.cols, total), BF16),
            pltpu.VMEM((plan.xrows, plan.cols), F32),
        ],
        cost=4,
    )
    got = exchange(grads)
    scale = pool / plan.batch
    count = n * plan.batch
    spot = jnp.stack([me * params.shape[0], last])
    base, old = call(
        functools.partial(prepare_kernel, plan),
        (spot, params.reshape(flat), momentum.reshape(flat), noise_draws.reshape(flat)),
        [(flat, F32), (flat, F32)],
        [pltpu.VMEM(flat, F32), pltpu.VMEM(flat, F32), pltpu.SemaphoreType.DMA((3,))],
        smem=1,
        whole=3,
    )
    new_params, new_momentum, loss = call(
        functools.partial(update_kernel, plan, scale, count),
        (spot, got, base, old),
        [(flat, F32), (flat, F32), ((1, LANES), F32)],
        [pltpu.VMEM(flat, F32)],
        smem=1,
    )
    return new_params.reshape(-1), new_momentum.reshape(-1), loss[0, :1]


def total_nll(flat_vec, din, chosen_rows, targets):
    in_end = din * H
    hid_end = in_end + H
    w_in = flat_vec[:in_end].reshape(din, H)
    b_in = flat_vec[in_end:hid_end]
    w_out = flat_vec[hid_end : hid_end + H * OUT].reshape(H, OUT)
    b_out = flat_vec[hid_end + H * OUT : hid_end + H * OUT + OUT]
    high = dict(precision=lax.Precision.HIGHEST, preferred_element_type=F32)
    hidden = jnp.tanh(jnp.dot(chosen_rows, w_in, **high) + b_in)
    logits = jnp.dot(hidden, w_out, **high) + b_out
    log_norm = jnp.log(jnp.sum(jnp.exp(logits), axis=1))
    classes = iota(logits.shape, 1)
    picked = jnp.sum(jnp.where(targets[:, None] == classes, logits, 0.0), axis=1)
    return jnp.sum(log_norm - picked)


def plain_body(params, momentum, noise_draws, images, labels, indices):
    shard_len = params.shape[0]
    din = images.shape[1]
    shard_start = lax.axis_index("dp") * shard_len
    precision = precision_of(shard_start + lax.iota(jnp.int32, shard_len), din)
    gathered = lax.all_gather(params, "dp", axis=0, tiled=True)
    chosen_rows = jnp.take(images, indices[0], axis=0)
    targets = jnp.take(labels, indices[0], axis=0)
    nll, pullback = jax.vjp(lambda w: total_nll(w, din, chosen_rows, targets), gathered)
    (local_grad,) = pullback(jnp.ones_like(nll))
    loss = lax.psum(nll, "dp") / (lax.axis_size("dp") * indices.shape[1])
    own_grad = lax.psum_scatter(local_grad, "dp", scatter_dimension=0, tiled=True)
    force = images.shape[0] / indices.shape[1] * own_grad + precision * params
    momentum = (1.0 - step_size * friction) * momentum - step_size * force
    momentum = momentum + math.sqrt(2.0 * friction * step_size) * noise_draws[0]
    return params + step_size * momentum, momentum, loss.reshape(1)


def solution(mesh):
    n = mesh.shape["dp"]

    def body(*args):
        params, images, indices = args[0], args[3], args[5]
        if Plan.fits(n, images.shape[1], params.shape[0], indices.shape[1]):
            return fast_body(n, *args)
        return plain_body(*args)

    placed = (
        P(("grp", "dp")),
        P(("grp", "dp")),
        P("grp", "dp"),
        P(("grp", "dp"), None),
        P(("grp", "dp")),
        P("grp", "dp"),
    )
    return jax.shard_map(
        body,
        mesh=mesh,
        in_specs=placed,
        out_specs=(P(("grp", "dp")), P(("grp", "dp")), P("grp")),
        check_vma=False,
    )
```

```python
import functools
import math

import jax
import jax.numpy as jnp
from jax import lax
from jax.experimental import pallas as pl
from jax.experimental.pallas import tpu as pltpu
from jax.sharding import PartitionSpec as P


H = 2048
OUT = 10
LANES = 128
SHARE = 0.72
COPIES = 2

step_size = 0.02
friction = 15.0
F32, BF16 = jnp.float32, jnp.bfloat16


def up8(n):
    return -(-n // 8) * 8


class Plan:
    def __init__(self, devices, din, shard_len, batch):
        self.n = devices
        self.group = devices // COPIES
        self.din = din
        self.cols = H // self.group
        self.nb = self.cols // LANES
        self.rows = shard_len // H
        self.unit = self.rows * self.nb
        self.back = self.unit + self.nb
        self.step = H // LANES
        self.early, self.middle, self.rest = (0, 2), (1, 3, 4), (5, 6, 7)
        self.flat = shard_len // LANES
        self.batch = batch
        self.tail = din + 1 - (devices - 1) * self.rows
        gcd = math.gcd(LANES, OUT)
        self.hp, self.qp = LANES // gcd, OUT // gcd
        self.periods = self.cols // self.hp
        self.classes = up8(OUT)
        self.xrows = -(-(din + 2) // 16) * 16
        first = round(SHARE * self.xrows / 16) * 16
        self.parts = (slice(0, first), slice(first, self.xrows))

    @staticmethod
    def fits(devices, din, shard_len, batch):
        if devices & (devices - 1) or devices < 2 * COPIES or shard_len % (8 * LANES) or shard_len % H:
            return False
        group, rows = devices // COPIES, shard_len // H
        if H % (group * LANES) or batch % LANES or group != 8 or din % 8:
            return False
        tail = din + 1 - (devices - 1) * rows
        return 0 < tail and tail + OUT + 1 <= rows


def split(x):
    hi = x.astype(BF16)
    return hi, (x - hi.astype(F32)).astype(BF16)


def split3(x):
    hi = x.astype(BF16)
    rest = x - hi.astype(F32)
    mid = rest.astype(BF16)
    return hi, mid, (rest - mid.astype(F32)).astype(BF16)


def dot(a, b, dims):
    return lax.dot_general(a, b, (dims, ((), ())), preferred_element_type=F32)


NN, NT = ((1,), (0,)), ((1,), (1,))


def iota(shape, axis):
    return lax.broadcasted_iota(jnp.int32, shape, axis)


def prior_kernel(plan, at_ref, out_ref):
    shape = (plan.flat, LANES)
    index = at_ref[0] + iota(shape, 0) * LANES + iota(shape, 1)
    out_ref[...] = precision_of(index, plan.din)


def pick_kernel(plan, img_ref, lab_ref, idx_ref, *parts):
    pool = img_ref.shape[1]
    hot = (iota((pool, plan.batch), 0) == idx_ref[...]).astype(BF16)
    hi, mid, lo = split3(img_ref[...])
    rows = dot(hi, hot, NN) + dot(mid, hot, NN) + dot(lo, hot, NN)
    spare = plan.xrows - plan.din
    marks = jnp.broadcast_to(lab_ref[...].astype(F32), (spare, pool)).astype(BF16)
    marks = dot(marks, hot, NN)
    at = iota((spare, plan.batch), 0)
    rows = jnp.concatenate([rows, jnp.where(at == 0, 1.0, jnp.where(at == 1, marks, 0.0))], axis=0)
    for part, ref in zip(plan.parts, parts):
        ref[...] = rows[part]


def cut_kernel(plan, last_ref, par_ref, out_ref):
    cut_weights(plan, last_ref, par_ref, out_ref)


def cut_weights(plan, last_ref, par_ref, out_ref):
    for j in range(plan.group):
        for b in range(plan.nb):
            piece = par_ref[pl.ds(j * plan.nb + b, plan.rows, stride=plan.step), :]
            for d in range(j, plan.n, plan.group):
                out_ref[pl.ds(d * plan.unit + b, plan.rows, stride=plan.nb), :] = piece

    @pl.when(last_ref[0] == 1)
    def _():
        t, count = plan.tail, OUT * plan.nb
        bias = par_ref[(t + OUT) * plan.step : (t + OUT) * plan.step + 1, :]
        for j in range(plan.group):
            start = t * plan.step + j * count
            piece = par_ref[start : start + count, :]
            for d in range(j, plan.n, plan.group):
                at = d * plan.unit + t * plan.nb
                out_ref[at : at + count, :] = piece
                out_ref[at + count : at + count + 1, :] = bias


def class_masks(plan):
    width = plan.qp * LANES
    mask = (iota((plan.classes, width), 1) % OUT == iota((plan.classes, width), 0)).astype(F32)
    place = (iota((width, plan.hp), 0) // OUT == iota((width, plan.hp), 1)).astype(BF16)
    return mask, place


def blocks_of(plan):
    return [(d, d * plan.rows, min(plan.rows, plan.din + 1 - d * plan.rows)) for d in range(plan.n)]


def out_weights(plan, w_ref, a_ref):
    mask, place = class_masks(plan)
    lhs = []
    for p in range(plan.periods):
        parts = []
        for q in range(plan.qp):
            row = (plan.n - 1) * plan.unit + plan.tail * plan.nb + p * plan.qp + q
            parts.append(jnp.broadcast_to(w_ref[row : row + 1, :], (plan.classes, LANES)))
        lhs.append(jnp.concatenate(parts, axis=1) * mask)
    hi, mid, lo = split3(jnp.concatenate(lhs, axis=0))
    out_w = dot(hi, place, NN) + dot(mid, place, NN) + dot(lo, place, NN)
    for p in range(plan.periods):
        rows = slice(p * plan.classes, (p + 1) * plan.classes)
        a_ref[:, p * plan.hp : (p + 1) * plan.hp] = out_w[rows]


def split_rows(plan, parts, x_ref, here):
    for part, ref in zip(plan.parts, parts):
        hi, lo = split(ref[...])
        x_ref[part, here] = hi
        x_ref[plan.xrows + part.start : plan.xrows + part.stop, here] = lo


def keep_labels(plan, m, ref, lab_ref):
    per = plan.batch // LANES
    mark = plan.din + 1 - plan.parts[1].start
    for i in range(per):
        row = ref[mark : mark + 1, i * LANES : (i + 1) * LANES]
        lab_ref[m * per + i : m * per + i + 1, :] = row


def forward_slots(plan, slots, x_ref, w_cat, a_cat, h_ref, own_ref, send_ref):
    per = plan.batch // LANES
    pre = dot(w_cat, x_ref[: plan.xrows, :], NN)
    pre = pre[: plan.cols] + (pre[plan.cols :] + dot(w_cat[: plan.cols], x_ref[plan.xrows :, :], NN))
    h_hi, h_lo = split(jnp.tanh(pre))
    h_ref[: plan.cols, :] = h_hi
    h_ref[plan.cols :, :] = h_lo
    lg = dot(a_cat, h_hi, NN)
    lg = lg[: plan.classes] + (lg[plan.classes :] + dot(a_cat[: plan.classes], h_lo, NN))
    for s, m in enumerate(slots):
        for i in range(per):
            own, other, at = m * per + i, (m ^ 1) * per + i, (s * per + i) * LANES
            block = lg[:OUT, at : at + LANES]
            own_ref[pl.ds(own, OUT, stride=plan.group * per), :] = block
            send_ref[pl.ds(other, OUT, stride=plan.group * per), :] = block


def ready_kernel(plan, *refs):
    join_ref, lab_ref = refs[-2:]
    lab_ref[...] = jnp.zeros_like(lab_ref)
    for s, m in enumerate(plan.early):
        pair = refs[2 * s : 2 * s + 2]
        keep_labels(plan, m, pair[1], lab_ref)
        for part, ref in zip(plan.parts, pair):
            join_ref[s, part, :] = ref[...]


def front_kernel(plan, w_ref, join_ref, x_ref, h_ref, a_ref, cat_ref, own_ref, send_ref, c_ref):
    out_weights(plan, w_ref, a_ref)
    a_cat = jnp.concatenate(split(a_ref[...]), axis=0)
    c_ref[...] = jnp.zeros_like(c_ref)
    for d, first, rows in blocks_of(plan):
        for b in range(plan.nb):
            piece = w_ref[pl.ds(d * plan.unit + b, rows, stride=plan.nb), :]
            c_ref[first : first + rows, b * LANES : (b + 1) * LANES] = piece
    w_cat = jnp.concatenate(split(c_ref[...].T), axis=0)
    cat_ref[...] = w_cat
    own_ref[...] = jnp.zeros_like(own_ref)
    send_ref[...] = jnp.zeros_like(send_ref)
    for s, m in enumerate(plan.early):
        here = slice(s * plan.batch, (s + 1) * plan.batch)
        x = split(join_ref[s])
        x_ref[: plan.xrows, here] = x[0]
        x_ref[plan.xrows :, here] = x[1]
    forward_slots(plan, plan.early, x_ref, w_cat, a_cat, h_ref, own_ref, send_ref)


def later_kernel(plan, slots, joined, cat_ref, a_ref, own1_ref, send1_ref, lab1_ref, *refs):
    x_ref, h_ref, own_ref, send_ref, lab_ref = refs[-5:]
    own_ref[...] = own1_ref[...]
    send_ref[...] = send1_ref[...]
    lab_ref[...] = lab1_ref[...]
    w_cat = cat_ref[...]
    a_cat = jnp.concatenate(split(a_ref[...]), axis=0)
    pairs = refs[min(joined, 1) : -5]
    for s, m in enumerate(slots):
        here = slice(s * plan.batch, (s + 1) * plan.batch)
        if s < joined:
            keep_labels(plan, m, refs[0].at[s, plan.parts[1].start :, :], lab_ref)
            x = split(refs[0][s])
            x_ref[: plan.xrows, here] = x[0]
            x_ref[plan.xrows :, here] = x[1]
        else:
            pair = pairs[2 * (s - joined) :][:2]
            keep_labels(plan, m, pair[1], lab_ref)
            split_rows(plan, pair, x_ref, here)
    forward_slots(plan, slots, x_ref, w_cat, a_cat, h_ref, own_ref, send_ref)


def backward_kernel(plan, own_ref, w_ref, a_ref, x1_ref, x2_ref, x3_ref, h1_ref, h2_ref, h3_ref, lab_ref, *refs):
    lg_refs, (out_ref, lg_ref, dl_ref, dh_ref, dw_ref) = refs[:-5], refs[-5:]
    per = plan.batch // LANES
    lines = plan.group * per
    order = (*plan.early, *plan.middle, *plan.rest)
    diag = iota((plan.classes, LANES), 0) == iota((plan.classes, LANES), 1)
    row = (plan.n - 1) * plan.unit + (plan.tail + OUT) * plan.nb
    bias = w_ref[row : row + 1, :]
    wide = 2 * per

    def placed(ref, o, q):
        at = [o * lines + (p ^ q) * wide for p in range(plan.group // 2)]
        return jnp.concatenate([ref[start : start + wide, :] for start in at], axis=0)

    values = []
    for o in range(OUT):
        value = own_ref[o * lines : (o + 1) * lines, :]
        for i, ref in enumerate(lg_refs):
            value = value + placed(ref, o, i + 1)
        values.append(value)
    labels = lab_ref[...].astype(jnp.int32)
    logits = [values[o] + bias[:, o : o + 1] for o in range(OUT)]
    top = functools.reduce(jnp.maximum, logits)
    ex = [jnp.exp(v - top) for v in logits]
    norm = functools.reduce(jnp.add, ex)
    hits = [labels == o for o in range(OUT)]
    picked = functools.reduce(jnp.add, [jnp.where(h, v, 0.0) for h, v in zip(hits, logits)])
    nll = jnp.sum(jnp.sum(jnp.log(norm) + top - picked, axis=1, keepdims=True), axis=0, keepdims=True)
    share = 1.0 / norm
    dl_ref[...] = jnp.zeros_like(dl_ref)
    for o in range(OUT):
        value = ex[o] * share - jnp.where(hits[o], 1.0, 0.0)
        lg_ref[o * lines : (o + 1) * lines, :] = value
    for i in range(lines):
        at = (order.index(i // per) * per + i % per) * LANES
        dl_ref[:OUT, at : at + LANES] = lg_ref[pl.ds(i, OUT, stride=lines), :]
    dl = dl_ref[...]
    dbias = jnp.sum(dl, axis=1, keepdims=True)
    dbias = jnp.sum(jnp.where(diag, dbias, 0.0), axis=0, keepdims=True)
    dl_hi, dl_lo = split(dl)
    dl_cat = jnp.concatenate([dl_hi, dl_lo], axis=0)
    dl_three = jnp.concatenate([dl_hi, dl_hi, dl_lo], axis=0)
    a_hi, a_lo = split(a_ref[...])
    a_three = jnp.concatenate([v.astype(F32) for v in (a_hi, a_lo, a_hi)], axis=0).T.astype(BF16)
    cols, xrows, classes = plan.cols, plan.xrows, plan.classes
    da, start = 0.0, 0
    for h_ref in (h1_ref, h2_ref, h3_ref):
        width = h_ref.shape[1]
        for at in range(0, width, plan.batch):
            here = slice(start + at, start + at + plan.batch)
            local = slice(at, at + plan.batch)
            hidden = h_ref[:cols, local].astype(F32) + h_ref[cols:, local].astype(F32)
            dh = dot(a_three, dl_three[:, here], NN)
            dh_hi, dh_lo = split(dh * (1.0 - hidden * hidden))
            dh_ref[:cols, here] = dh_hi
            dh_ref[cols:, here] = dh_lo
        da = da + dot(h_ref[...], dl_cat[:, start : start + width], NT)
        start += width
    dw, start = 0.0, 0
    for x_ref in (x1_ref, x2_ref, x3_ref):
        here = slice(start, start + x_ref.shape[1])
        part = dot(x_ref[...], dh_ref[:cols, here], NT)
        dw = dw + (part[:xrows] + (part[xrows:] + dot(x_ref[:xrows, :], dh_ref[cols:, here], NT)))
        start = here.stop
    dw_ref[...] = dw
    out_ref[...] = jnp.zeros_like(out_ref)
    for d, first, count in blocks_of(plan):
        for b in range(plan.nb):
            piece = dw_ref[first : first + count, b * LANES : (b + 1) * LANES]
            out_ref[pl.ds(d * plan.back + b, count, stride=plan.nb), :] = piece
    da = da.T
    da = da[:classes, :cols] + (da[classes:, :cols] + da[:classes, cols:])
    mask, place = class_masks(plan)
    hi, mid, lo = split3(da)
    parts = []
    for v in (hi, mid, lo):
        parts.append(jnp.concatenate([v[:, p * plan.hp : (p + 1) * plan.hp] for p in range(plan.periods)], axis=0))
    back = dot(parts[0], place, NT) + dot(parts[1], place, NT) + dot(parts[2], place, NT)
    for p in range(plan.periods):
        line = jnp.sum(back[p * plan.classes : (p + 1) * plan.classes] * mask, axis=0, keepdims=True)
        for q in range(plan.qp):
            r = (plan.n - 1) * plan.back + plan.tail * plan.nb + p * plan.qp + q
            out_ref[r : r + 1, :] = line[:, q * LANES : (q + 1) * LANES]
    row = (plan.n - 1) * plan.back + (plan.tail + OUT) * plan.nb
    out_ref[row : row + 1, :] = dbias
    for d in range(plan.n):
        at = d * plan.back + plan.unit
        out_ref[at : at + 1, :] = jnp.broadcast_to(nll, (1, LANES))


def prepare_kernel(prior_ref, par_ref, mom_ref, noise_ref, base_ref, keep_ref, mom, noise, sems):
    loads = [pltpu.make_async_copy(s, d, sems.at[i]) for i, (s, d) in enumerate(
        ((par_ref, keep_ref), (mom_ref, mom), (noise_ref, noise)))]
    for load in loads:
        load.start()
    for load in loads:
        load.wait()
    prior = prior_ref[...] * keep_ref[...]
    base = (1.0 - step_size * friction) * mom[...] - step_size * prior
    base_ref[...] = base + math.sqrt(2.0 * friction * step_size) * noise[...]


def update_kernel(plan, scale, count, at_ref, got_ref, base_ref, par_ref, par_out, mom_out, loss_ref, grad_ref):
    def summed(j, start, size, stride=1):
        total = 0.0
        for g in range(COPIES):
            at = (g * plan.group + j) * plan.back + start
            total = total + got_ref[pl.ds(at, size, stride=stride), :]
        return total

    for j in range(plan.group):
        for b in range(plan.nb):
            spot = pl.ds(j * plan.nb + b, plan.rows, stride=plan.step)
            grad_ref[spot, :] = summed(j, b, plan.rows, plan.nb)
    loss_ref[...] = summed(0, plan.unit, 1) * (1.0 / count)

    @pl.when(at_ref[1] == 1)
    def _():
        t, size = plan.tail, OUT * plan.nb
        row = (t + OUT) * plan.step
        grad_ref[row:, :] = jnp.zeros((plan.flat - row, LANES), F32)
        grad_ref[row : row + 1, :] = summed(0, (t + OUT) * plan.nb, 1)
        for j in range(plan.group):
            at = t * plan.step + j * size
            grad_ref[at : at + size, :] = summed(j, t * plan.nb, size)

    mom = base_ref[...] - (step_size * scale) * grad_ref[...]
    mom_out[...] = mom
    par_out[...] = par_ref[...] + step_size * mom


def precision_of(index, din):
    in_end = din * H
    hid_end = in_end + H
    out_end = hid_end + H * OUT
    inner = jnp.where(index < hid_end, 1.0, jnp.where(index < out_end, float(H), 1.0))
    return jnp.where(index < in_end, float(din), inner)


def call(kernel, args, outs, scratch=(), smem=0, limit=16, whole=0, cost=1, lead=0):
    vm = pl.BlockSpec(memory_space=pltpu.VMEM)
    sm = pl.BlockSpec(memory_space=pltpu.SMEM)
    anywhere = pl.BlockSpec(memory_space=pltpu.HBM)
    specs = [sm] * smem + [vm] * lead + [anywhere] * whole
    return pl.pallas_call(
        kernel,
        out_shape=[jax.ShapeDtypeStruct(s, t) for s, t in outs],
        in_specs=specs + [vm] * (len(args) - len(specs)),
        out_specs=[vm] * len(outs),
        scratch_shapes=list(scratch),
        compiler_params=pltpu.CompilerParams(vmem_limit_bytes=limit << 20),
        cost_estimate=pl.CostEstimate(flops=cost * 10**9, bytes_accessed=1 << 20, transcendentals=0),
    )(*args)


def fast_body(n, params, momentum, noise_draws, images, labels, indices):
    pool, din = images.shape
    plan = Plan(n, din, params.shape[0], indices.shape[1])
    me = lax.axis_index("dp")
    last = (me == n - 1).astype(jnp.int32)
    flat = (plan.flat, LANES)

    def exchange(x):
        x = x.reshape(n, -1, plan.nb, LANES)
        return lax.all_to_all(x, "dp", 0, 0, tiled=True).reshape(-1, LANES)

    total = plan.group * plan.batch
    lines = total // LANES
    dense = (OUT * lines, LANES)

    def hop(x, k):
        return lax.ppermute(x, "dp", [(d, d ^ k) for d in range(n)])


    (prior,) = call(
        functools.partial(prior_kernel, plan),
        ((me * params.shape[0]).reshape(1),),
        [(flat, F32)],
        smem=1,
        cost=3,
    )
    a, b = call(
        functools.partial(pick_kernel, plan),
        (images.T, labels.reshape(1, pool), indices),
        [((part.stop - part.start, plan.batch), F32) for part in plan.parts],
    )
    b2 = hop(b, 2)
    a4 = hop(a, 4)
    a2 = hop(a, 2)
    b4 = hop(b, 4)
    a6 = hop(a4, 2)
    b6 = hop(b2, 4)
    (cut,) = call(
        functools.partial(cut_kernel, plan),
        (last.reshape(1), params.reshape(flat)),
        [((n * plan.unit, LANES), F32)],
        smem=1,
    )
    weights = exchange(cut)
    half = len(plan.early) * plan.batch
    join, marks = call(
        functools.partial(ready_kernel, plan),
        (a, b, a2, b2),
        [((len(plan.early), plan.xrows, plan.batch), F32), ((lines, LANES), F32)],
    )
    weights, join = lax.optimization_barrier((weights, join))
    other = hop(join, 1)
    x1, h1, outw, cat, own, send = call(
        functools.partial(front_kernel, plan),
        (weights, join),
        [
            ((2 * plan.xrows, half), BF16),
            ((2 * plan.cols, half), BF16),
            ((plan.classes, plan.cols), F32),
            ((2 * plan.cols, plan.xrows), BF16),
            (dense, F32),
            (dense, F32),
        ],
        [pltpu.VMEM((plan.xrows, plan.cols), F32)],
        cost=3,
    )

    def later(slots, joined, *args):
        width = len(slots) * plan.batch
        return call(
            functools.partial(later_kernel, plan, slots, joined),
            (cat, outw, own, send, marks, *args),
            [
                ((2 * plan.xrows, width), BF16),
                ((2 * plan.cols, width), BF16),
                (dense, F32),
                (dense, F32),
                ((lines, LANES), F32),
            ],
            cost=2,
        )

    a5, b5 = hop(a4, 1), hop(b4, 1)
    outw, a6, b6 = lax.optimization_barrier((outw, a6, b6))
    a7, b7 = hop(a6, 1), hop(b6, 1)
    x2, h2, own, send, marks = later(plan.middle, len(plan.early), other, a4, b4)
    x3, h3, own, send, marks = later(plan.rest, 0, a5, b5, a6, b6, a7, b7)
    own = own + hop(send, 1)
    more = [hop(own, k) for k in range(2, plan.group, 2)]
    (grads,) = call(
        functools.partial(backward_kernel, plan),
        (own, weights, outw, x1, x2, x3, h1, h2, h3, marks, *more),
        [((n * plan.back, LANES), F32)],
        [
            pltpu.VMEM(dense, F32),
            pltpu.VMEM((plan.classes, total), F32),
            pltpu.VMEM((2 * plan.cols, total), BF16),
            pltpu.VMEM((plan.xrows, plan.cols), F32),
        ],
        cost=4,
    )
    got = exchange(grads)
    scale = pool / plan.batch
    count = n * plan.batch
    spot = jnp.stack([me * params.shape[0], last])
    base, old = call(
        prepare_kernel,
        (prior, params.reshape(flat), momentum.reshape(flat), noise_draws.reshape(flat)),
        [(flat, F32), (flat, F32)],
        [pltpu.VMEM(flat, F32), pltpu.VMEM(flat, F32), pltpu.SemaphoreType.DMA((3,))],
        lead=1,
        whole=3,
    )
    new_params, new_momentum, loss = call(
        functools.partial(update_kernel, plan, scale, count),
        (spot, got, base, old),
        [(flat, F32), (flat, F32), ((1, LANES), F32)],
        [pltpu.VMEM(flat, F32)],
        smem=1,
    )
    return new_params.reshape(-1), new_momentum.reshape(-1), loss[0, :1]


def total_nll(flat_vec, din, chosen_rows, targets):
    in_end = din * H
    hid_end = in_end + H
    w_in = flat_vec[:in_end].reshape(din, H)
    b_in = flat_vec[in_end:hid_end]
    w_out = flat_vec[hid_end : hid_end + H * OUT].reshape(H, OUT)
    b_out = flat_vec[hid_end + H * OUT : hid_end + H * OUT + OUT]
    high = dict(precision=lax.Precision.HIGHEST, preferred_element_type=F32)
    hidden = jnp.tanh(jnp.dot(chosen_rows, w_in, **high) + b_in)
    logits = jnp.dot(hidden, w_out, **high) + b_out
    log_norm = jnp.log(jnp.sum(jnp.exp(logits), axis=1))
    classes = iota(logits.shape, 1)
    picked = jnp.sum(jnp.where(targets[:, None] == classes, logits, 0.0), axis=1)
    return jnp.sum(log_norm - picked)


def plain_body(params, momentum, noise_draws, images, labels, indices):
    shard_len = params.shape[0]
    din = images.shape[1]
    shard_start = lax.axis_index("dp") * shard_len
    precision = precision_of(shard_start + lax.iota(jnp.int32, shard_len), din)
    gathered = lax.all_gather(params, "dp", axis=0, tiled=True)
    chosen_rows = jnp.take(images, indices[0], axis=0)
    targets = jnp.take(labels, indices[0], axis=0)
    nll, pullback = jax.vjp(lambda w: total_nll(w, din, chosen_rows, targets), gathered)
    (local_grad,) = pullback(jnp.ones_like(nll))
    loss = lax.psum(nll, "dp") / (lax.axis_size("dp") * indices.shape[1])
    own_grad = lax.psum_scatter(local_grad, "dp", scatter_dimension=0, tiled=True)
    force = images.shape[0] / indices.shape[1] * own_grad + precision * params
    momentum = (1.0 - step_size * friction) * momentum - step_size * force
    momentum = momentum + math.sqrt(2.0 * friction * step_size) * noise_draws[0]
    return params + step_size * momentum, momentum, loss.reshape(1)


def solution(mesh):
    n = mesh.shape["dp"]

    def body(*args):
        params, images, indices = args[0], args[3], args[5]
        if Plan.fits(n, images.shape[1], params.shape[0], indices.shape[1]):
            return fast_body(n, *args)
        return plain_body(*args)

    placed = (
        P(("grp", "dp")),
        P(("grp", "dp")),
        P("grp", "dp"),
        P(("grp", "dp"), None),
        P(("grp", "dp")),
        P("grp", "dp"),
    )
    return jax.shard_map(
        body,
        mesh=mesh,
        in_specs=placed,
        out_specs=(P(("grp", "dp")), P(("grp", "dp")), P("grp")),
        check_vma=False,
    )
```
